512 devices in a mesh: replica: 32 (over z, x_hi, core), expert: 16 (over x_lo, y).
Axes of the slice: x: 4 (x_hi: 2, x_lo: 2; x = x_hi * 2 + x_lo), y: 8, z: 8, core: 2. Of those that a mesh axis runs over, the one named last changes fastest.
Arguments:
- tokens: float32 [98304, 2048], P(('replica', 'expert')), may hold values from -6 to 6
- expert_ids: int32 [98304, 2], P(('replica', 'expert')), may hold values from 0 to 15, all different within a row; in each aligned block of 192 rows (0 to 191, 192 to 383, ...) at most 36 rows name the same one
- combine_weights: float32 [98304, 2], P(('replica', 'expert')), may hold values from 0.3 to 1
- gate_weight: bfloat16 [16, 2048, 768], P('expert', 'replica'), may hold values from -0.125 to 0.125
- up_weight: bfloat16 [16, 2048, 768], P('expert', 'replica'), may hold values from -0.125 to 0.125
- down_weight: bfloat16 [16, 2048, 768], P('expert', 'replica'), may hold values from -0.21875 to 0.21875
- norm_gain: float32 [2048], replicated, may hold values from 0.1 to 1.9
Outputs:
- normed: float32 [98304, 2048], P(('replica', 'expert'))
The draws below stay inside these ranges and needn't reach their ends.
Inputs may be any that keep to these rules, and one draw needn't show every extreme that they name: `expert_ids`: each row names two different experts. In each aligned block of 192 rows (the rows of one device) no expert is named by more than 36 rows, a bound that some block reaches.
All inputs are finite; a program needn't handle non-finite values.
Results may differ from the reference program's by a relative error of at most 0.0027.
Values may be sent and summed in bfloat16 or wider, within the bound.
A program may use at most 64 MiB of HBM per device.

```python
import math
import jax
import jax.numpy as jnp
import numpy as np
from jax import lax

D = 2048
FF = 768
TOK_DEV = 192
EXPERTS = 16
CAP = 36
TOKENS = 98304
N_REPLICA = 32
N_EXPERT = 16


def block_levels(stream_key, extent, pieces, low, top_value):
    level, own = 1.0, jax.random.fold_in(stream_key, 6)
    for axis_at, parts in pieces:
        draws = jnp.exp(jax.random.uniform(jax.random.fold_in(own, axis_at), (parts,), jnp.float32, low / len(pieces), top_value / len(pieces)))
        level = level * jnp.repeat(draws, extent[axis_at] // parts).reshape([-1 if axis == axis_at else 1 for axis in range(len(extent))])
    return level


def deal_out(own_key, own, number, rows, number_of, top, limit, slope):
    sequence = jax.random.permutation(own_key, number_of)
    packed, common = portions_of(number_of, rows * top, limit, slope, True), portions_of(number_of, rows * top, limit, slope, False)
    places = jnp.arange(number_of)

    def named(tallies, offset_by):
        used = int((tallies > 0).sum())
        fixed = max(1, used // 4)
        shifted = fixed + (places - fixed + offset_by * (used - fixed)) % max(1, number_of - fixed)
        return jnp.zeros((number_of,), jnp.int32).at[sequence[jnp.where(places < fixed, places, shifted)]].set(jnp.asarray(tallies, jnp.int32))

    tallies = jnp.where(number % 4 == 0, named(packed, number // 4), named(common, number - number // 4 - 1))
    mixed = jax.random.permutation(jax.random.fold_in(own, 3), number_of)
    donor, taker = mixed[0:number_of // 2 * 2:2], mixed[1:number_of // 2 * 2:2]
    slack = jnp.minimum(tallies[donor] - 1, limit - tallies[taker]) // 2
    slack = jnp.where((donor == sequence[0]) | (taker == sequence[0]) | (tallies[taker] == 0), 0, jnp.maximum(slack, 0))
    shifted = jax.random.randint(jax.random.fold_in(own, 4), (number_of // 2,), 0, 1 << 20) % (slack + 1)
    tallies = tallies.at[donor].add(-shifted).at[taker].add(shifted)
    items = jnp.searchsorted(jnp.cumsum(tallies), jnp.arange(rows * top), side="right").astype(jnp.int32)
    table = items.reshape(top, rows).T
    table = table[jax.random.permutation(jax.random.fold_in(own, 1), rows)]
    offset_by = jax.random.randint(jax.random.fold_in(own, 2), (rows, 1), 0, top)
    return jnp.take_along_axis(table, (jnp.arange(top)[None, :] + offset_by) % top, axis=1)


def portions_of(amount, total, reach, skew, full):
    loads = [(1 << 20) // math.isqrt(grade ** skew) + 1 for grade in range(1, amount + 1)]
    largest = reach if full else min(reach, max(-(-total // amount), total * loads[0] // sum(loads)))
    least = 1 if total - largest >= amount - 1 else 0
    counts, surplus = [largest] + [least] * (amount - 1), total - largest - least * (amount - 1)
    while surplus > 0:
        free = [i for i in range(1, amount) if counts[i] < largest] or [i for i in range(1, amount) if counts[i] < reach]
        whole, budget = sum([loads[i] for i in free]), surplus
        for i in free:
            addition = min(reach - counts[i], max(1, budget * loads[i] // whole), surplus)
            counts[i] = counts[i] + addition
            surplus = surplus - addition
    return np.array(counts)


def scatter_about(own_key, dims, scale, limit, split=(), held_as=jnp.bfloat16):
    level = block_levels(own_key, dims, split, -0.22, 0.18) if split else 1.0
    array = jax.random.normal(own_key, dims, jnp.float32) * scale * level
    return jnp.minimum(jnp.maximum(array, -limit), limit).astype(held_as)


def setup_inputs(seed: int = 0) -> dict:
    splits = jax.random.split(jax.random.key(seed), 8)
    tokens = scatter_about(splits[0], (TOKENS, D), 1.0, 6.0, ((0, 512),), jnp.float32)
    expert_ids_keys = jax.random.split(jax.random.fold_in(splits[1], 1), TOKENS // TOK_DEV)
    expert_ids_turns = jax.random.permutation(jax.random.fold_in(splits[1], 3), TOKENS // TOK_DEV)
    expert_ids = jax.vmap(lambda own, number: deal_out(jax.random.fold_in(splits[1], 2), own, number, TOK_DEV, EXPERTS, 2, CAP, 2))(expert_ids_keys, expert_ids_turns).reshape((TOKENS, 2))
    combine_weights = jnp.clip(0.3 + 0.7 * jax.random.uniform(splits[2], (TOKENS, 2), jnp.float32) ** block_levels(splits[2], (TOKENS, 2), ((0, 512),), -0.2, 0.2), 0.3, 1.0)
    gate_weight = scatter_about(splits[3], (EXPERTS, D, FF), D ** -0.5, 0.125, ((0, 16), (1, 32)))
    up_weight = scatter_about(splits[4], (EXPERTS, D, FF), D ** -0.5, 0.125, ((0, 16), (1, 32)))
    down_weight = scatter_about(splits[5], (EXPERTS, D, FF), FF ** -0.5, 0.21875, ((0, 16), (1, 32)))
    norm_gain = jnp.clip(1.0 + 0.18 * jax.random.normal(splits[6], (D,), jnp.float32), 0.1, 1.9)
    return dict(tokens=tokens, expert_ids=expert_ids, combine_weights=combine_weights, gate_weight=gate_weight, up_weight=up_weight, down_weight=down_weight, norm_gain=norm_gain)


def slot_positions(expert_ids, experts, capacity):
    count = expert_ids.shape[0]
    onehot = (expert_ids[:, :, None] == jnp.arange(experts, dtype=jnp.int32)[None, None, :]).astype(jnp.int32)
    onehot = onehot.reshape(count * 2, experts)
    before = jnp.cumsum(onehot, axis=0) - onehot
    ranks = lax.optimization_barrier(jnp.sum(before * onehot, axis=1)).reshape(count, 2)
    return (expert_ids * capacity + ranks).astype(jnp.int32)

def place_rows(tokens, slot_index, total):
    iota_slots = jnp.arange(total, dtype=jnp.int32)[:, None]
    select = (slot_index[None, :, 0] == iota_slots) | (slot_index[None, :, 1] == iota_slots)
    return jnp.dot(select.astype(jnp.bfloat16), tokens.astype(jnp.bfloat16), preferred_element_type=jnp.float32).astype(jnp.bfloat16)

def expert_ffn(rows, gate, upward, downward):
    gate_out = jnp.dot(rows, gate, preferred_element_type=jnp.float32)
    up_out = jnp.dot(rows, upward, preferred_element_type=jnp.float32)
    hidden = (jax.nn.silu(gate_out) * up_out).astype(jnp.bfloat16)
    result = lax.dot_general(hidden, downward, (((1,), (1,)), ((), ())), preferred_element_type=jnp.float32)
    return result.astype(jnp.bfloat16)

def combine_rows(tokens, back, slot_index, weights, gain):
    picked = back[slot_index].astype(jnp.float32)
    summed = lax.optimization_barrier(jnp.sum(picked * weights[:, :, None], axis=1))
    mixed = tokens + summed
    scale = lax.rsqrt(lax.optimization_barrier(jnp.mean(mixed * mixed, axis=-1)) + 1e-06)
    return mixed * scale[:, None] * gain[None, :]

def reference(tokens, expert_ids, combine_weights, gate_weight, up_weight, down_weight, norm_gain):
    groups = N_EXPERT
    capacity = 3 * TOK_DEV // EXPERTS
    tok_blocks = tokens.reshape(N_REPLICA, groups, TOK_DEV, D)
    id_blocks = expert_ids.reshape(N_REPLICA, groups, TOK_DEV, 2)
    weight_blocks = combine_weights.reshape(N_REPLICA, groups, TOK_DEV, 2)

    def one_replica(inputs):
        toks, idents, weights = inputs
        slot_index = jax.vmap(lambda ids: slot_positions(ids, EXPERTS, capacity))(idents)
        placed = jax.vmap(lambda t, s: place_rows(t, s, EXPERTS * capacity))(toks, slot_index)
        rows = placed.reshape(groups, EXPERTS, capacity, D).transpose(1, 0, 2, 3).reshape(EXPERTS, groups * capacity, D)
        outs = lax.map(lambda a: expert_ffn(a[0], a[1], a[2], a[3]), (rows, gate_weight, up_weight, down_weight))
        back = outs.reshape(EXPERTS, groups, capacity, D).transpose(1, 0, 2, 3).reshape(groups, EXPERTS * capacity, D)
        return jax.vmap(lambda t, b, s, w: combine_rows(t, b, s, w, norm_gain))(toks, back, slot_index, weights)
    result = lax.map(one_replica, (tok_blocks, id_blocks, weight_blocks))
    return result.reshape(TOKENS, D)
```

```python
import jax
import jax.numpy as jnp
from jax import lax
from jax.experimental import pallas as pl
from jax.experimental.pallas import tpu as pltpu
from jax.sharding import PartitionSpec as P

MESH = pl.DeviceIdType.MESH
BF = jnp.bfloat16
F32 = jnp.float32

TOK = 192
WIDTH = 2048
FF = 768
CAP = 36
MAIN = 32
TAIL = CAP - MAIN
GROUPS = 4
COLS = WIDTH // GROUPS
ROWS = GROUPS * CAP
SHARD = 64
PIECES = 3


def hop_y(k, dx):
    far = 2 if dx < 2 else 6
    one = k * (2 - k) * (3 - k) // 2
    two = k * (k - 1) * (3 - k) // 2
    three = k * (k - 1) * (k - 2) // 6
    return one + 7 * two + far * three


def where_am_i():
    r = lax.axis_index("replica")
    e = lax.axis_index("expert")
    z = r // 4
    xh = (r // 2) % 2
    core = r % 2
    xl = e // 8
    y = e % 8
    return xh * 2 + xl, y, z, core


def device(x, y, z, core):
    return ((z * 2 + x // 2) * 2 + core, (x % 2) * 8 + y)


def partner_of(ids, x, y):
    host_x = (ids >> 3) + 2 * ((ids >> 2) & 1)
    dx = (host_x - x) & 3
    d4 = ((ids & 3) - y) & 3
    k = d4 ^ (d4 >> 1)
    return ((k - dx - 1) & 3) * 4 + dx


def iota(shape, dim):
    return lax.broadcasted_iota(jnp.int32, shape, dim)


def kernel(
    tok_hbm, ids_ref, idst_ref, cw_ref, gate_hbm, up_hbm, down_hbm,
    mixed_ref,
    tok, w, send, recv, eout, back, whi, wlo, thi, tlo,
    tok_sem, pre_send, pre_recv, ring_send, ring_recv, sib_send, sib_recv,
    out_send, out_recv, ret_send, ret_recv,
):
    x, y, z, core = where_am_i()
    xh = x // 2
    mine = z * 4 + xh * 2 + core
    home = xh == y // 4
    shards = (gate_hbm, up_hbm, down_hbm)

    tok_copy = pltpu.make_async_copy(tok_hbm, tok, tok_sem)
    tok_copy.start()

    offsets = [(dx, dy) for dx in range(4) for dy in (0, 1, 7)]
    offsets += [(0, 2), (0, 6), (1, 2), (2, 2), (2, 6), (3, 6)]
    offsets += [(0, 4), (2, 4)]
    greet = [device((x + dx) % 4, (y + dy) % 8, z, core) for dx, dy in offsets if (dx, dy) != (0, 0)]
    greet += [device(x, y, z, 1 - core), device(x, y, (z + 1) % 8, core), device(x, y, (z + 7) % 8, core)]
    barrier = pltpu.get_barrier_semaphore()
    for d in greet:
        pl.semaphore_signal(barrier, inc=1, device_id=d, device_id_type=MESH)
    pl.semaphore_wait(barrier, len(greet))

    def piece(slot, p):
        return w.at[slot, pl.ds(p * SHARD, SHARD), :]

    def push_own(p, d):
        pltpu.make_async_remote_copy(
            src_ref=shards[p].at[0], dst_ref=piece(mine, p),
            send_sem=pre_send, recv_sem=pre_recv.at[xh, p],
            device_id=d, device_id_type=MESH,
        ).start()

    @pl.when(home)
    def _():
        for p in range(PIECES):
            pltpu.make_async_copy(shards[p].at[0], piece(mine, p), pre_recv.at[xh, p]).start()
            push_own(p, device(x, (y + 4) % 8, z, core))

    @pl.when(jnp.logical_not(home))
    def _():
        for p in range(PIECES):
            push_own(p, device((x + 2) % 4, (y + 4) % 8, z, core))
            push_own(p, device((x + 2) % 4, y, z, core))

    tok_copy.wait()
    q0 = partner_of(idst_ref[0:1, :], x, y)
    q1 = partner_of(idst_ref[1:2, :], x, y)
    hot0 = (q0 == iota((16, TOK), 0)).astype(F32)
    hot1 = (q1 == iota((16, TOK), 0)).astype(F32)
    upper = (iota((TOK, TOK), 0) < iota((TOK, TOK), 1)).astype(BF)
    count = jnp.dot((hot0 + hot1).astype(BF), upper, preferred_element_type=F32)
    rank0 = jnp.sum(hot0 * count, axis=0, keepdims=True).astype(jnp.int32)
    rank1 = jnp.sum(hot1 * count, axis=0, keepdims=True).astype(jnp.int32)
    main0 = jnp.where(rank0 < MAIN, q0 * MAIN + rank0, -1)
    main1 = jnp.where(rank1 < MAIN, q1 * MAIN + rank1, -1)
    tail0 = jnp.where(rank0 < MAIN, -1000, q0 * 16 + rank0 - MAIN)
    tail1 = jnp.where(rank1 < MAIN, -1000, q1 * 16 + rank1 - MAIN)
    select = jnp.where((main0 == iota((16 * MAIN, TOK), 0)) | (main1 == iota((16 * MAIN, TOK), 0)), 1.0, 0.0).astype(BF)
    tails = jnp.zeros((256, COLS), F32)
    for c in range(GROUPS):
        tok_c = tok[:, c * COLS:(c + 1) * COLS].astype(BF)
        placed = jnp.dot(select, tok_c, preferred_element_type=F32).astype(BF)
        send[:, c * MAIN:(c + 1) * MAIN, :] = placed.reshape(16, MAIN, COLS)
        at = iota((256, TOK), 0) - 4 * c
        pick = jnp.where((tail0 == at) | (tail1 == at), 1.0, 0.0).astype(BF)
        tails += jnp.dot(pick, tok_c, preferred_element_type=F32)
    send[:, GROUPS * MAIN:, :] = tails.astype(BF).reshape(16, 16, COLS)

    def message(q, buf_from, buf_to, sem_from, sem_to, d):
        return pltpu.make_async_remote_copy(
            src_ref=buf_from.at[q], dst_ref=buf_to.at[q], send_sem=sem_from, recv_sem=sem_to,
            device_id=d, device_id_type=MESH,
        )

    for g in range(4):
        for dx in range(4):
            q = g * 4 + dx
            dy = hop_y((g + 1 + dx) % 4, dx)
            if (dx, dy) != (0, 0):
                message(q, send, recv, out_send, out_recv, device((x + dx) % 4, (y + dy) % 8, z, core)).start()
    recv[12] = send[12]

    p0 = partner_of(ids_ref[:, 0:1], x, y)
    p1 = partner_of(ids_ref[:, 1:2], x, y)
    col0 = (p0 == iota((TOK, 16), 1)).astype(F32)
    col1 = (p1 == iota((TOK, 16), 1)).astype(F32)
    lower = (iota((TOK, TOK), 1) < iota((TOK, TOK), 0)).astype(BF)
    ccount = jnp.dot(lower, (col0 + col1).astype(BF), preferred_element_type=F32)
    crank0 = jnp.sum(col0 * ccount, axis=1, keepdims=True).astype(jnp.int32)
    crank1 = jnp.sum(col1 * ccount, axis=1, keepdims=True).astype(jnp.int32)
    cw0 = cw_ref[:, 0:1]
    cw1 = cw_ref[:, 1:2]
    cmain0 = jnp.where(crank0 < MAIN, p0 * MAIN + crank0, -1)
    cmain1 = jnp.where(crank1 < MAIN, p1 * MAIN + crank1, -1)
    ctail0 = jnp.where(crank0 < MAIN, -1000, p0 * 16 + crank0 - MAIN)
    ctail1 = jnp.where(crank1 < MAIN, -1000, p1 * 16 + crank1 - MAIN)
    slots = iota((TOK, 16 * MAIN), 1)
    full = jnp.where(cmain0 == slots, cw0, 0.0) + jnp.where(cmain1 == slots, cw1, 0.0)
    high = full.astype(BF)
    whi[...] = high
    wlo[...] = (full - high.astype(F32)).astype(BF)
    for c in range(GROUPS):
        slots = iota((TOK, 256), 1) - 4 * c
        full = jnp.where(ctail0 == slots, cw0, 0.0) + jnp.where(ctail1 == slots, cw1, 0.0)
        high = full.astype(BF)
        thi[c] = high
        tlo[c] = (full - high.astype(F32)).astype(BF)

    def ring(step, way, hx, p, slot):
        d = device(x, y, (z + (1 if way == 0 else 7)) % 8, core)
        return pltpu.make_async_remote_copy(
            src_ref=piece(slot, p), dst_ref=piece(slot, p),
            send_sem=ring_send, recv_sem=ring_recv.at[((step * 2 + way) * 2 + hx) * PIECES + p],
            device_id=d, device_id_type=MESH,
        )

    def sibling(p, slot, from_z):
        return pltpu.make_async_remote_copy(
            src_ref=piece(slot, p), dst_ref=piece(slot, p),
            send_sem=sib_send, recv_sem=sib_recv.at[from_z],
            device_id=device(x, y, z, 1 - core), device_id_type=MESH,
        )

    for p in range(PIECES):
        for turn in range(2):
            hx = xh if turn == 0 else 1 - xh
            slot = z * 4 + hx * 2 + core
            pltpu.make_async_copy(piece(slot, p), piece(slot, p), pre_recv.at[hx, p]).wait()
            for way in range(2):
                d = device(x, y, (z + (1 if way == 0 else 7)) % 8, core)
                pltpu.make_async_remote_copy(
                    src_ref=piece(slot, p), dst_ref=piece(slot, p),
                    send_sem=ring_send, recv_sem=ring_recv.at[(way * 2 + hx) * PIECES + p],
                    device_id=d, device_id_type=MESH,
                ).start()
            sibling(p, slot, z).start()

    for step in range(4):
        for p in range(PIECES):
            for hx in range(2):
                for way in range(2):
                    if step == 3 and way != hx:
                        continue
                    origin = (z + (7 - step if way == 0 else 1 + step)) % 8
                    slot = origin * 4 + hx * 2 + core
                    ring(step, way, hx, p, slot).wait_recv()
                    if step < 2 or (step == 2 and way == hx):
                        ring(step + 1, way, hx, p, slot).start()
                    sibling(p, slot, origin).start()

    pltpu.make_async_copy(recv.at[0:15], recv.at[0:15], out_recv).wait()
    for k in range(8):
        pltpu.make_async_copy(w.at[0:2], w.at[0:2], sib_recv.at[k]).wait()

    def spread(c):
        a = iota((16, 64), 0)
        b = iota((16, 64), 1)
        return jnp.where((a // 4 == b // 16) & (a % 4 == b % 4) & ((b // 4) % 4 == c), 1.0, 0.0).astype(BF)

    def gather(c):
        a = iota((64, 16), 1)
        b = iota((64, 16), 0)
        return jnp.where((a // 4 == b // 16) & (a % 4 == b % 4) & ((b // 4) % 4 == c), 1.0, 0.0).astype(BF)

    def chunk(g, carry):
        base = pl.multiple_of(g * 4, 4)
        last = recv[pl.ds(base, 4), GROUPS * MAIN:, :].reshape(64, COLS)
        gate = jnp.zeros((4 * CAP, FF), F32)
        upward = jnp.zeros((4 * CAP, FF), F32)
        for c in range(GROUPS):
            main = recv[pl.ds(base, 4), c * MAIN:(c + 1) * MAIN, :].reshape(4 * MAIN, COLS)
            rest = jnp.dot(spread(c), last, preferred_element_type=F32).astype(BF)
            rows = jnp.concatenate([main, rest], axis=0)
            gate += jnp.dot(rows, w[c * 8:(c + 1) * 8, 0:SHARD, :].reshape(COLS, FF), preferred_element_type=F32)
            upward += jnp.dot(rows, w[c * 8:(c + 1) * 8, SHARD:2 * SHARD, :].reshape(COLS, FF), preferred_element_type=F32)
        hidden = (gate / (1.0 + jnp.exp(-gate)) * upward).astype(BF)
        rests = jnp.zeros((64, COLS), F32)
        for c in range(GROUPS):
            down = w[c * 8:(c + 1) * 8, 2 * SHARD:, :].reshape(COLS, FF)
            res = lax.dot_general(hidden, down, (((1,), (1,)), ((), ())), preferred_element_type=F32).astype(BF)
            eout[pl.ds(base, 4), c * MAIN:(c + 1) * MAIN, :] = res[:4 * MAIN].reshape(4, MAIN, COLS)
            rests += jnp.dot(gather(c), res[4 * MAIN:], preferred_element_type=F32)
        eout[pl.ds(base, 4), GROUPS * MAIN:, :] = rests.astype(BF).reshape(4, 16, COLS)
        for dx in range(4):
            dy = hop_y((g + 1 + dx) % 4, dx)
            back_to = device((x + 4 - dx) % 4, (y + 8 - dy) % 8, z, core)
            if dx == 0:
                @pl.when(g < 3)
                def _():
                    message(base + dx, eout, back, ret_send, ret_recv, back_to).start()
            else:
                message(base + dx, eout, back, ret_send, ret_recv, back_to).start()
        return carry

    lax.fori_loop(0, 4, chunk, 0)
    back[12] = eout[12]
    pltpu.make_async_copy(back.at[0:15], back.at[0:15], ret_recv).wait()

    last = back[:, GROUPS * MAIN:, :].reshape(256, COLS)
    for c in range(GROUPS):
        main = back[:, c * MAIN:(c + 1) * MAIN, :].reshape(16 * MAIN, COLS)
        total = jnp.dot(whi[...], main, preferred_element_type=F32)
        total += jnp.dot(wlo[...], main, preferred_element_type=F32)
        total += jnp.dot(thi[c], last, preferred_element_type=F32)
        total += jnp.dot(tlo[c], last, preferred_element_type=F32)
        mixed_ref[:, c * COLS:(c + 1) * COLS] = tok[:, c * COLS:(c + 1) * COLS] + total

    @pl.when(home)
    def _():
        pltpu.make_async_copy(w.at[0], w.at[0], pre_send).wait()

    @pl.when(jnp.logical_not(home))
    def _():
        pltpu.make_async_copy(w.at[0:2], w.at[0:2], pre_send).wait()

    pltpu.make_async_copy(w.at[0:14], w.at[0:14], ring_send).wait()
    pltpu.make_async_copy(w.at[0:16], w.at[0:16], sib_send).wait()
    pltpu.make_async_copy(send.at[0:15], send.at[0:15], out_send).wait()
    pltpu.make_async_copy(eout.at[0:15], eout.at[0:15], ret_send).wait()


def on_device(tokens, expert_ids, combine_weights, gate_weight, up_weight, down_weight, norm_gain):
    anywhere = pl.BlockSpec(memory_space=pl.ANY)
    vmem = pl.BlockSpec(memory_space=pltpu.VMEM)
    dma = pltpu.SemaphoreType.DMA
    mixed = pl.pallas_call(
        kernel,
        out_shape=jax.ShapeDtypeStruct((TOK, WIDTH), F32),
        in_specs=[anywhere, vmem, vmem, vmem, anywhere, anywhere, anywhere],
        out_specs=vmem,
        scratch_shapes=[
            pltpu.VMEM((TOK, WIDTH), F32),
            pltpu.VMEM((32, PIECES * SHARD, FF), BF),
            pltpu.VMEM((16, ROWS, COLS), BF),
            pltpu.VMEM((16, ROWS, COLS), BF),
            pltpu.VMEM((16, ROWS, COLS), BF),
            pltpu.VMEM((16, ROWS, COLS), BF),
            pltpu.VMEM((TOK, 16 * MAIN), BF),
            pltpu.VMEM((TOK, 16 * MAIN), BF),
            pltpu.VMEM((GROUPS, TOK, 256), BF),
            pltpu.VMEM((GROUPS, TOK, 256), BF),
            dma, dma, dma((2, PIECES)), dma, dma((16 * PIECES,)), dma, dma((8,)),
            dma, dma, dma, dma,
        ],
        compiler_params=pltpu.CompilerParams(
            collective_id=0, has_side_effects=True, vmem_limit_bytes=48 << 20
        ),
        cost_estimate=pl.CostEstimate(flops=7_000_000_000, bytes_accessed=30_000_000, transcendentals=500_000),
    )(tokens, expert_ids, expert_ids.T, combine_weights, gate_weight, up_weight, down_weight)
    scale = lax.rsqrt(jnp.mean(mixed * mixed, axis=-1) + 1e-06)
    return mixed * scale[:, None] * norm_gain[None, :]


def solution(mesh):
    placed = (
        P(("replica", "expert"), None),
        P(("replica", "expert"), None),
        P(("replica", "expert"), None),
        P("expert", "replica", None),
        P("expert", "replica", None),
        P("expert", "replica", None),
        P(),
    )
    return jax.shard_map(
        on_device,
        mesh=mesh,
        in_specs=placed,
        out_specs=P(("replica", "expert"), None),
        check_vma=False,
    )
```

```python
import jax
import jax.numpy as jnp
from jax import lax
from jax.experimental import pallas as pl
from jax.experimental.pallas import tpu as pltpu
from jax.sharding import PartitionSpec as P

MESH = pl.DeviceIdType.MESH
BF = jnp.bfloat16
F32 = jnp.float32

TOK = 192
WIDTH = 2048
FF = 768
CAP = 36
MAIN = 32
TAIL = CAP - MAIN
GROUPS = 4
COLS = WIDTH // GROUPS
ROWS = GROUPS * CAP
SHARD = 64
PIECES = 3
SELF = 12


def hop_y(k, dx):
    far = 2 if dx < 2 else 6
    one = k * (2 - k) * (3 - k) // 2
    two = k * (k - 1) * (3 - k) // 2
    three = k * (k - 1) * (k - 2) // 6
    return one + 7 * two + far * three


def where_am_i():
    r = lax.axis_index("replica")
    e = lax.axis_index("expert")
    z = r // 4
    xh = (r // 2) % 2
    core = r % 2
    xl = e // 8
    y = e % 8
    return xh * 2 + xl, y, z, core


def device(x, y, z, core):
    return ((z * 2 + x // 2) * 2 + core, (x % 2) * 8 + y)


def partner_of(ids, x, y):
    host_x = (ids >> 3) + 2 * ((ids >> 2) & 1)
    dx = (host_x - x) & 3
    d4 = ((ids & 3) - y) & 3
    k = d4 ^ (d4 >> 1)
    return ((k - dx - 1) & 3) * 4 + dx


def iota(shape, dim):
    return lax.broadcasted_iota(jnp.int32, shape, dim)


def kernel(
    tok_hbm, ids_hbm, cw_hbm, gate_hbm, up_hbm, down_hbm,
    mixed_ref,
    tok, ids_ref, cw_ref, wgu, wd, send, recv, hid, eout, back, whi, wlo, thi, tlo,
    in_sem, pre_send, pre_recv, ring_send, ring_recv, down_recv, sib_send, sib_gu, sib_down,
    out_send, out_recv, ret_send, ret_recv,
):
    x, y, z, core = where_am_i()
    xh = x // 2
    mine = z * 4 + xh * 2 + core
    home = xh == y // 4
    shards = (gate_hbm, up_hbm, down_hbm)

    ids_copy = pltpu.make_async_copy(ids_hbm, ids_ref, in_sem.at[0])
    cw_copy = pltpu.make_async_copy(cw_hbm, cw_ref, in_sem.at[1])
    tok_copy = pltpu.make_async_copy(tok_hbm, tok, in_sem.at[2])
    ids_copy.start()
    cw_copy.start()
    tok_copy.start()

    offsets = [(dx, dy) for dx in range(4) for dy in (0, 1, 7)]
    offsets += [(0, 2), (0, 6), (1, 2), (2, 2), (2, 6), (3, 6)]
    offsets += [(0, 4), (2, 4)]
    greet = [device((x + dx) % 4, (y + dy) % 8, z, core) for dx, dy in offsets if (dx, dy) != (0, 0)]
    other = device(x, y, z, 1 - core)
    sides = (device(x, y, (z + 1) % 8, core), device(x, y, (z + 7) % 8, core))
    greet += [other, sides[0], sides[1]]
    barrier = pltpu.get_barrier_semaphore()
    for d in greet:
        pl.semaphore_signal(barrier, inc=1, device_id=d, device_id_type=MESH)
    pl.semaphore_wait(barrier, len(greet))

    def piece(slot, p):
        return wd.at[slot] if p == 2 else wgu.at[slot, pl.ds(p * SHARD, SHARD), :]

    def remote(src, dst, sem_from, sem_to, d):
        return pltpu.make_async_remote_copy(
            src_ref=src, dst_ref=dst, send_sem=sem_from, recv_sem=sem_to, device_id=d, device_id_type=MESH
        )

    def push_own(p, d):
        remote(shards[p].at[0], piece(mine, p), pre_send.at[p // 2], pre_recv.at[xh, p], d).start()

    @pl.when(home)
    def _():
        for p in range(PIECES):
            pltpu.make_async_copy(shards[p].at[0], piece(mine, p), pre_recv.at[xh, p]).start()
            push_own(p, device(x, (y + 4) % 8, z, core))

    @pl.when(jnp.logical_not(home))
    def _():
        for p in range(PIECES):
            push_own(p, device((x + 2) % 4, (y + 4) % 8, z, core))
            push_own(p, device((x + 2) % 4, y, z, core))

    ids_copy.wait()
    cw_copy.wait()
    tok_copy.wait()
    q0 = partner_of(ids_ref[0:1, :], x, y)
    q1 = partner_of(ids_ref[1:2, :], x, y)
    hot0 = (q0 == iota((16, TOK), 0)).astype(F32)
    hot1 = (q1 == iota((16, TOK), 0)).astype(F32)
    upper = (iota((TOK, TOK), 0) < iota((TOK, TOK), 1)).astype(BF)
    count = jnp.dot((hot0 + hot1).astype(BF), upper, preferred_element_type=F32)
    rank0 = jnp.sum(hot0 * count, axis=0, keepdims=True).astype(jnp.int32)
    rank1 = jnp.sum(hot1 * count, axis=0, keepdims=True).astype(jnp.int32)
    main0 = jnp.where(rank0 < MAIN, q0 * MAIN + rank0, -1)
    main1 = jnp.where(rank1 < MAIN, q1 * MAIN + rank1, -1)
    tail0 = jnp.where(rank0 < MAIN, -1000, q0 * 16 + rank0 - MAIN)
    tail1 = jnp.where(rank1 < MAIN, -1000, q1 * 16 + rank1 - MAIN)
    select = jnp.where((main0 == iota((16 * MAIN, TOK), 0)) | (main1 == iota((16 * MAIN, TOK), 0)), 1.0, 0.0).astype(BF)
    tails = jnp.zeros((256, COLS), F32)
    for c in range(GROUPS):
        tok_c = tok[:, c * COLS:(c + 1) * COLS].astype(BF)
        placed = jnp.dot(select, tok_c, preferred_element_type=F32).astype(BF)
        send[:, c * MAIN:(c + 1) * MAIN, :] = placed.reshape(16, MAIN, COLS)
        at = iota((256, TOK), 0) - 4 * c
        pick = jnp.where((tail0 == at) | (tail1 == at), 1.0, 0.0).astype(BF)
        tails += jnp.dot(pick, tok_c, preferred_element_type=F32)
    send[:, GROUPS * MAIN:, :] = tails.astype(BF).reshape(16, 16, COLS)

    partners = []
    for g in range(4):
        for dx in range(4):
            dy = hop_y((g + 1 + dx) % 4, dx)
            if (dx, dy) != (0, 0):
                partners.append((g * 4 + dx, dx, dy))
    for q, dx, dy in partners:
        remote(send.at[q], recv.at[q], out_send, out_recv, device((x + dx) % 4, (y + dy) % 8, z, core)).start()
    recv[SELF] = send[SELF]

    def arrival(step, way, hx, p):
        if p == 2:
            return down_recv.at[(step * 2 + way) * 2 + hx]
        return ring_recv.at[((step * 2 + way) * 2 + hx) * 2 + p]

    def onward(step, way, hx, p, slot):
        return remote(piece(slot, p), piece(slot, p), ring_send.at[p // 2], arrival(step, way, hx, p), sides[way])

    def sibling(p, slot, from_z):
        sem = sib_down.at[from_z] if p == 2 else sib_gu
        remote(piece(slot, p), piece(slot, p), sib_send.at[p // 2], sem, other).start()

    def own_turn(p):
        for turn in range(2):
            hx = xh if turn == 0 else 1 - xh
            slot = z * 4 + hx * 2 + core
            pltpu.make_async_copy(piece(slot, p), piece(slot, p), pre_recv.at[hx, p]).wait()
            for way in range(2):
                onward(0, way, hx, p, slot).start()
            sibling(p, slot, z)

    def ring_turn(step, pieces):
        for p in pieces:
            for hx in range(2):
                for way in range(2):
                    if step == 3 and way != hx:
                        continue
                    origin = (z + (7 - step if way == 0 else 1 + step)) % 8
                    slot = origin * 4 + hx * 2 + core
                    onward(step, way, hx, p, slot).wait_recv()
                    if step < 2 or (step == 2 and way == hx):
                        onward(step + 1, way, hx, p, slot).start()
                    sibling(p, slot, origin)

    own_turn(0)
    own_turn(1)
    ring_turn(0, (0, 1))

    diagonal = iota((TOK, TOK), 0) == iota((TOK, TOK), 1)

    def column(row):
        return jnp.sum(jnp.where(diagonal, row, 0.0), axis=1, keepdims=True)

    cw0 = column(cw_ref[0:1, :])
    cw1 = column(cw_ref[1:2, :])
    cmain0 = column(main0.astype(F32)).astype(jnp.int32)
    cmain1 = column(main1.astype(F32)).astype(jnp.int32)
    ctail0 = column(tail0.astype(F32)).astype(jnp.int32)
    ctail1 = column(tail1.astype(F32)).astype(jnp.int32)
    slots = iota((TOK, 16 * MAIN), 1)
    full = jnp.where(cmain0 == slots, cw0, 0.0) + jnp.where(cmain1 == slots, cw1, 0.0)
    high = full.astype(BF)
    whi[...] = high
    wlo[...] = (full - high.astype(F32)).astype(BF)
    for c in range(GROUPS):
        slots = iota((TOK, 256), 1) - 4 * c
        full = jnp.where(ctail0 == slots, cw0, 0.0) + jnp.where(ctail1 == slots, cw1, 0.0)
        high = full.astype(BF)
        thi[c] = high
        tlo[c] = (full - high.astype(F32)).astype(BF)

    ring_turn(1, (0, 1))
    ring_turn(2, (0, 1))
    own_turn(2)
    ring_turn(3, (0, 1))
    pltpu.make_async_copy(recv.at[0:15], recv.at[0:15], out_recv).wait()
    pltpu.make_async_copy(wgu.at[0:16], wgu.at[0:16], sib_gu).wait()

    def spread(c):
        a = iota((16, 64), 0)
        b = iota((16, 64), 1)
        return jnp.where((a // 4 == b // 16) & (a % 4 == b % 4) & ((b // 4) % 4 == c), 1.0, 0.0).astype(BF)

    def chunk(g, carry):
        base = pl.multiple_of(g * 4, 4)
        last = recv[pl.ds(base, 4), GROUPS * MAIN:, :].reshape(64, COLS)
        gate = jnp.zeros((4 * CAP, FF), F32)
        upward = jnp.zeros((4 * CAP, FF), F32)
        for c in range(GROUPS):
            main = recv[pl.ds(base, 4), c * MAIN:(c + 1) * MAIN, :].reshape(4 * MAIN, COLS)
            rest = jnp.dot(spread(c), last, preferred_element_type=F32).astype(BF)
            rows = jnp.concatenate([main, rest], axis=0)
            gate += jnp.dot(rows, wgu[c * 8:(c + 1) * 8, 0:SHARD, :].reshape(COLS, FF), preferred_element_type=F32)
            upward += jnp.dot(rows, wgu[c * 8:(c + 1) * 8, SHARD:, :].reshape(COLS, FF), preferred_element_type=F32)
        units = (gate / (1.0 + jnp.exp(-gate)) * upward).astype(BF)
        hid[pl.ds(pl.multiple_of(g * 128, 128), 128), :] = units[:128]
        hid[pl.ds(pl.multiple_of(512 + g * 16, 16), 16), :] = units[128:]
        return carry

    def pair(j):
        return ((z + (7 - j)) % 8, (z + 1 + j) % 8) if j < 3 else (z, (z + 4) % 8)

    def gather(s):
        a = iota((256, 64), 0)
        b = iota((256, 64), 1)
        return jnp.where((a // 16 == b // 4) & (a % 4 == b % 4) & ((a // 4) % 4 == s), 1.0, 0.0).astype(BF)

    def columns(j):
        rests = jnp.zeros((256, 128), F32)
        for half, origin in enumerate(pair(j)):
            pltpu.make_async_copy(wd.at[0:2], wd.at[0:2], sib_down.at[origin]).wait()
            down = wd[pl.ds(pl.multiple_of(origin * 4, 4), 4)].reshape(256, FF)
            res = lax.dot_general(hid[...], down, (((1,), (1,)), ((), ())), preferred_element_type=F32).astype(BF)
            for part in range(2):
                s = half * 2 + part
                lanes = res[:, part * 128:(part + 1) * 128]
                eout[j, :, s * MAIN:(s + 1) * MAIN, :] = lanes[:512].reshape(16, MAIN, 128)
                rests += jnp.dot(gather(s), lanes[512:], preferred_element_type=F32)
        eout[j, :, GROUPS * MAIN:, :] = rests.astype(BF).reshape(16, 16, 128)
        for q, dx, dy in partners:
            back_to = device((x + 4 - dx) % 4, (y + 8 - dy) % 8, z, core)
            remote(eout.at[j, q], back.at[j, q], ret_send.at[j], ret_recv.at[j], back_to).start()
        back[j, SELF] = eout[j, SELF]

    lax.fori_loop(0, 2, chunk, 0)
    ring_turn(0, (2,))
    lax.fori_loop(2, 4, chunk, 0)
    ring_turn(1, (2,))
    columns(0)
    ring_turn(2, (2,))
    columns(1)
    ring_turn(3, (2,))
    columns(2)
    columns(3)

    for j in range(4):
        pltpu.make_async_copy(back.at[j, 0:15], back.at[j, 0:15], ret_recv.at[j]).wait()
        last = back[j, :, GROUPS * MAIN:, :].reshape(256, 128)
        main = jnp.concatenate(
            [back[j, :, s * MAIN:(s + 1) * MAIN, :].reshape(16 * MAIN, 128) for s in range(4)], axis=1
        )
        total = jnp.dot(whi[...], main, preferred_element_type=F32)
        total += jnp.dot(wlo[...], main, preferred_element_type=F32)
        total += jnp.concatenate(
            [
                jnp.dot(thi[s], last, preferred_element_type=F32) + jnp.dot(tlo[s], last, preferred_element_type=F32)
                for s in range(4)
            ],
            axis=1,
        )
        for half, origin in enumerate(pair(j)):
            at = pl.ds(pl.multiple_of(origin * 256, 256), 256)
            mixed_ref[:, at] = tok[:, at] + total[:, half * 256:(half + 1) * 256]

    @pl.when(home)
    def _():
        pltpu.make_async_copy(wgu.at[0], wgu.at[0], pre_send.at[0]).wait()
        pltpu.make_async_copy(wd.at[0], wd.at[0], pre_send.at[1]).wait()

    @pl.when(jnp.logical_not(home))
    def _():
        pltpu.make_async_copy(wgu.at[0:2], wgu.at[0:2], pre_send.at[0]).wait()
        pltpu.make_async_copy(wd.at[0:2], wd.at[0:2], pre_send.at[1]).wait()

    pltpu.make_async_copy(wgu.at[0:14], wgu.at[0:14], ring_send.at[0]).wait()
    pltpu.make_async_copy(wd.at[0:14], wd.at[0:14], ring_send.at[1]).wait()
    pltpu.make_async_copy(wgu.at[0:16], wgu.at[0:16], sib_send.at[0]).wait()
    pltpu.make_async_copy(wd.at[0:16], wd.at[0:16], sib_send.at[1]).wait()
    pltpu.make_async_copy(send.at[0:15], send.at[0:15], out_send).wait()
    for j in range(4):
        pltpu.make_async_copy(eout.at[j, 0:15], eout.at[j, 0:15], ret_send.at[j]).wait()


def on_device(tokens, expert_ids, combine_weights, gate_weight, up_weight, down_weight, norm_gain):
    hbm = pl.BlockSpec(memory_space=pltpu.HBM)
    vmem = pl.BlockSpec(memory_space=pltpu.VMEM)
    dma = pltpu.SemaphoreType.DMA
    mixed = pl.pallas_call(
        kernel,
        out_shape=jax.ShapeDtypeStruct((TOK, WIDTH), F32),
        in_specs=[hbm] * 6,
        out_specs=vmem,
        scratch_shapes=[
            pltpu.VMEM((TOK, WIDTH), F32),
            pltpu.VMEM((2, TOK), jnp.int32),
            pltpu.VMEM((2, TOK), F32),
            pltpu.VMEM((32, 2 * SHARD, FF), BF),
            pltpu.VMEM((32, SHARD, FF), BF),
            pltpu.VMEM((16, ROWS, COLS), BF),
            pltpu.VMEM((16, ROWS, COLS), BF),
            pltpu.VMEM((16 * CAP, FF), BF),
            pltpu.VMEM((4, 16, ROWS, 128), BF),
            pltpu.VMEM((4, 16, ROWS, 128), BF),
            pltpu.VMEM((TOK, 16 * MAIN), BF),
            pltpu.VMEM((TOK, 16 * MAIN), BF),
            pltpu.VMEM((GROUPS, TOK, 256), BF),
            pltpu.VMEM((GROUPS, TOK, 256), BF),
            dma((3,)), dma((2,)), dma((2, PIECES)), dma((2,)), dma((32,)), dma((16,)), dma((2,)), dma, dma((8,)),
            dma, dma, dma((4,)), dma((4,)),
        ],
        compiler_params=pltpu.CompilerParams(
            collective_id=0, has_side_effects=True, vmem_limit_bytes=62500000
        ),
        cost_estimate=pl.CostEstimate(flops=7_000_000_000, bytes_accessed=30_000_000, transcendentals=500_000),
    )(tokens, expert_ids.T, combine_weights.T, gate_weight, up_weight, down_weight)
    scale = lax.rsqrt(jnp.mean(mixed * mixed, axis=-1) + 1e-06)
    return mixed * scale[:, None] * norm_gain[None, :]


def solution(mesh):
    placed = (
        P(("replica", "expert"), None),
        P(("replica", "expert"), None),
        P(("replica", "expert"), None),
        P("expert", "replica", None),
        P("expert", "replica", None),
        P("expert", "replica", None),
        P(),
    )
    return jax.shard_map(
        on_device,
        mesh=mesh,
        in_specs=placed,
        out_specs=P(("replica", "expert"), None),
        check_vma=False,
    )
```

```python
import jax
import jax.numpy as jnp
from jax import lax
from jax.experimental import pallas as pl
from jax.experimental.pallas import tpu as pltpu
from jax.sharding import PartitionSpec as P

MESH = pl.DeviceIdType.MESH
BF = jnp.bfloat16
F32 = jnp.float32

TOK = 192
WIDTH = 2048
FF = 768
CAP = 36
MAIN = 32
TAIL = CAP - MAIN
GROUPS = 4
COLS = WIDTH // GROUPS
ROWS = GROUPS * CAP
SHARD = 64
PIECES = 3
SELF = 12
HALF = 8 * CAP
HALF_MAIN = 8 * MAIN
HALF_TAIL = 8 * TAIL


def hop_y(k, dx):
    far = 2 if dx < 2 else 6
    one = k * (2 - k) * (3 - k) // 2
    two = k * (k - 1) * (3 - k) // 2
    three = k * (k - 1) * (k - 2) // 6
    return one + 7 * two + far * three


def where_am_i():
    r = lax.axis_index("replica")
    e = lax.axis_index("expert")
    z = r // 4
    xh = (r // 2) % 2
    core = r % 2
    xl = e // 8
    y = e % 8
    return xh * 2 + xl, y, z, core


def device(x, y, z, core):
    return ((z * 2 + x // 2) * 2 + core, (x % 2) * 8 + y)


def partner_of(ids, x, y):
    host_x = (ids >> 3) + 2 * ((ids >> 2) & 1)
    dx = (host_x - x) & 3
    d4 = ((ids & 3) - y) & 3
    k = d4 ^ (d4 >> 1)
    return ((k - dx - 1) & 3) * 4 + dx


def iota(shape, dim):
    return lax.broadcasted_iota(jnp.int32, shape, dim)


def kernel(
    tok_hbm, ids_hbm, cw_hbm, gate_hbm, up_hbm, down_hbm,
    mixed_hbm, scale_ref,
    tok, ids_ref, cw_ref, wgu, wd, send, recv, lhs, gacc, uacc, hid, eout, back, whi, wlo, thi, tlo,
    in_sem, res_sem, pre_send, pre_recv, ring_send, ring_recv, down_recv, sib_send, sib_gu, sib_down,
    out_send, out_recv, ret_send, ret_recv,
):
    x, y, z, core = where_am_i()
    xh = x // 2
    mine = z * 4 + xh * 2 + core
    home = xh == y // 4
    shards = (gate_hbm, up_hbm, down_hbm)

    ids_copy = pltpu.make_async_copy(ids_hbm, ids_ref, in_sem.at[0])
    cw_copy = pltpu.make_async_copy(cw_hbm, cw_ref, in_sem.at[1])
    tok_copy = pltpu.make_async_copy(tok_hbm, tok, in_sem.at[2])
    ids_copy.start()
    cw_copy.start()
    tok_copy.start()

    offsets = [(dx, dy) for dx in range(4) for dy in (0, 1, 7)]
    offsets += [(0, 2), (0, 6), (1, 2), (2, 2), (2, 6), (3, 6)]
    offsets += [(0, 4), (2, 4)]
    greet = [device((x + dx) % 4, (y + dy) % 8, z, core) for dx, dy in offsets if (dx, dy) != (0, 0)]
    other = device(x, y, z, 1 - core)
    sides = (device(x, y, (z + 1) % 8, core), device(x, y, (z + 7) % 8, core))
    greet += [other, sides[0], sides[1]]
    barrier = pltpu.get_barrier_semaphore()
    for d in greet:
        pl.semaphore_signal(barrier, inc=1, device_id=d, device_id_type=MESH)
    pl.semaphore_wait(barrier, len(greet))

    def piece(slot, p):
        return wd.at[slot] if p == 2 else wgu.at[slot, pl.ds(p * SHARD, SHARD), :]

    def remote(src, dst, sem_from, sem_to, d):
        return pltpu.make_async_remote_copy(
            src_ref=src, dst_ref=dst, send_sem=sem_from, recv_sem=sem_to, device_id=d, device_id_type=MESH
        )

    def push_own(p, d):
        remote(shards[p].at[0], piece(mine, p), pre_send.at[p // 2], pre_recv.at[xh, p], d).start()

    @pl.when(home)
    def _():
        for p in range(PIECES):
            pltpu.make_async_copy(shards[p].at[0], piece(mine, p), pre_recv.at[xh, p]).start()
            push_own(p, device(x, (y + 4) % 8, z, core))

    @pl.when(jnp.logical_not(home))
    def _():
        for p in range(PIECES):
            push_own(p, device((x + 2) % 4, (y + 4) % 8, z, core))
            push_own(p, device((x + 2) % 4, y, z, core))

    ids_copy.wait()
    cw_copy.wait()
    tok_copy.wait()
    q0 = partner_of(ids_ref[0:1, :], x, y)
    q1 = partner_of(ids_ref[1:2, :], x, y)
    hot0 = (q0 == iota((16, TOK), 0)).astype(F32)
    hot1 = (q1 == iota((16, TOK), 0)).astype(F32)
    upper = (iota((TOK, TOK), 0) < iota((TOK, TOK), 1)).astype(BF)
    count = jnp.dot((hot0 + hot1).astype(BF), upper, preferred_element_type=F32)
    rank0 = jnp.sum(hot0 * count, axis=0, keepdims=True).astype(jnp.int32)
    rank1 = jnp.sum(hot1 * count, axis=0, keepdims=True).astype(jnp.int32)
    main0 = jnp.where(rank0 < MAIN, q0 * MAIN + rank0, -1)
    main1 = jnp.where(rank1 < MAIN, q1 * MAIN + rank1, -1)
    tail0 = jnp.where(rank0 < MAIN, -1000, q0 * 16 + rank0 - MAIN)
    tail1 = jnp.where(rank1 < MAIN, -1000, q1 * 16 + rank1 - MAIN)
    select = jnp.where((main0 == iota((16 * MAIN, TOK), 0)) | (main1 == iota((16 * MAIN, TOK), 0)), 1.0, 0.0).astype(BF)
    tails = jnp.zeros((256, COLS), F32)
    for c in range(GROUPS):
        tok_c = tok[:, c * COLS:(c + 1) * COLS].astype(BF)
        placed = jnp.dot(select, tok_c, preferred_element_type=F32).astype(BF)
        send[:, c * MAIN:(c + 1) * MAIN, :] = placed.reshape(16, MAIN, COLS)
        at = iota((256, TOK), 0) - 4 * c
        pick = jnp.where((tail0 == at) | (tail1 == at), 1.0, 0.0).astype(BF)
        tails += jnp.dot(pick, tok_c, preferred_element_type=F32)
    send[:, GROUPS * MAIN:, :] = tails.astype(BF).reshape(16, 16, COLS)

    partners = []
    for g in range(4):
        for dx in range(4):
            dy = hop_y((g + 1 + dx) % 4, dx)
            if (dx, dy) != (0, 0):
                partners.append((g * 4 + dx, dx, dy))
    for q, dx, dy in partners:
        remote(send.at[q], recv.at[q], out_send, out_recv.at[q // 8], device((x + dx) % 4, (y + dy) % 8, z, core)).start()
    recv[SELF] = send[SELF]

    def arrival(step, way, hx, p):
        if p == 2:
            return down_recv.at[(step * 2 + way) * 2 + hx]
        return ring_recv.at[((step * 2 + way) * 2 + hx) * 2 + p]

    def onward(step, way, hx, p, slot):
        return remote(piece(slot, p), piece(slot, p), ring_send.at[p // 2], arrival(step, way, hx, p), sides[way])

    def sibling(p, slot, from_z):
        sem = sib_down.at[from_z] if p == 2 else sib_gu.at[from_z]
        remote(piece(slot, p), piece(slot, p), sib_send.at[p // 2], sem, other).start()

    def own_turn(p):
        for turn in range(2):
            hx = xh if turn == 0 else 1 - xh
            slot = z * 4 + hx * 2 + core
            pltpu.make_async_copy(piece(slot, p), piece(slot, p), pre_recv.at[hx, p]).wait()
            for way in range(2):
                onward(0, way, hx, p, slot).start()
            sibling(p, slot, z)

    def ring_turn(step, pieces):
        for p in pieces:
            for hx in range(2):
                for way in range(2):
                    if step == 3 and way != hx:
                        continue
                    origin = (z + (7 - step if way == 0 else 1 + step)) % 8
                    slot = origin * 4 + hx * 2 + core
                    onward(step, way, hx, p, slot).wait_recv()
                    if step < 2 or (step == 2 and way == hx):
                        onward(step + 1, way, hx, p, slot).start()
                    sibling(p, slot, origin)

    own_turn(0)
    own_turn(1)
    ring_turn(0, (0, 1))

    diagonal = iota((TOK, TOK), 0) == iota((TOK, TOK), 1)

    def column(row):
        return jnp.sum(jnp.where(diagonal, row, 0.0), axis=1, keepdims=True)

    cw0 = column(cw_ref[0:1, :])
    cw1 = column(cw_ref[1:2, :])
    cmain0 = column(main0.astype(F32)).astype(jnp.int32)
    cmain1 = column(main1.astype(F32)).astype(jnp.int32)
    ctail0 = column(tail0.astype(F32)).astype(jnp.int32)
    ctail1 = column(tail1.astype(F32)).astype(jnp.int32)
    slots = iota((TOK, 16 * MAIN), 1)
    full = jnp.where(cmain0 == slots, cw0, 0.0) + jnp.where(cmain1 == slots, cw1, 0.0)
    high = full.astype(BF)
    whi[...] = high
    wlo[...] = (full - high.astype(F32)).astype(BF)
    for c in range(GROUPS):
        slots = iota((TOK, 256), 1) - 4 * c
        full = jnp.where(ctail0 == slots, cw0, 0.0) + jnp.where(ctail1 == slots, cw1, 0.0)
        high = full.astype(BF)
        thi[c] = high
        tlo[c] = (full - high.astype(F32)).astype(BF)

    def spread(c):
        a = iota((HALF_TAIL, 128), 0)
        b = iota((HALF_TAIL, 128), 1)
        return jnp.where((a // 4 == b // 16) & (a % 4 == b % 4) & ((b // 4) % 4 == c), 1.0, 0.0).astype(BF)

    def unpack(h):
        got = recv.at[0:8 - h]
        pltpu.make_async_copy(got, got, out_recv.at[h]).wait()
        last = recv[h * 8:h * 8 + 8, GROUPS * MAIN:, :].reshape(128, COLS)
        for c in range(GROUPS):
            main = recv[h * 8:h * 8 + 8, c * MAIN:(c + 1) * MAIN, :].reshape(HALF_MAIN, COLS)
            rest = jnp.dot(spread(c), last, preferred_element_type=F32).astype(BF)
            for part in range(2):
                lanes = slice(part * 256, (part + 1) * 256)
                lhs[c * 2 + part, h * HALF:h * HALF + HALF_MAIN, :] = main[:, lanes]
                lhs[c * 2 + part, h * HALF + HALF_MAIN:(h + 1) * HALF, :] = rest[:, lanes]

    def weights_of(origin, p):
        at = pl.ds(pl.multiple_of(origin * 4, 4), 4)
        return wgu[at, p * SHARD:(p + 1) * SHARD, :].reshape(256, FF)

    def product(h, p, origins):
        rows = jnp.concatenate([lhs[o, h * HALF:(h + 1) * HALF, :] for o in origins], axis=1)
        return jnp.dot(rows, jnp.concatenate([weights_of(o, p) for o in origins], axis=0), preferred_element_type=F32)

    def activate(h, gate, upward):
        hid[h * HALF:(h + 1) * HALF, :] = (gate / (1.0 + jnp.exp(-gate)) * upward).astype(BF)

    def crossed(origin):
        pltpu.make_async_copy(wgu.at[0:2], wgu.at[0:2], sib_gu.at[origin]).wait()

    def pair(j):
        return ((z + (7 - j)) % 8, (z + 1 + j) % 8) if j < 3 else (z, (z + 4) % 8)

    def gather(s):
        a = iota((128, HALF_TAIL), 0)
        b = iota((128, HALF_TAIL), 1)
        return jnp.where((a // 16 == b // 4) & (a % 4 == b % 4) & ((a // 4) % 4 == s), 1.0, 0.0).astype(BF)

    def columns(j, h):
        rests = jnp.zeros((128, 128), F32)
        for half, origin in enumerate(pair(j)):
            if h == 0:
                pltpu.make_async_copy(wd.at[0:2], wd.at[0:2], sib_down.at[origin]).wait()
            down = wd[pl.ds(pl.multiple_of(origin * 4, 4), 4)].reshape(256, FF)
            res = lax.dot_general(
                hid[h * HALF:(h + 1) * HALF, :], down, (((1,), (1,)), ((), ())), preferred_element_type=F32
            ).astype(BF)
            for part in range(2):
                s = half * 2 + part
                lanes = res[:, part * 128:(part + 1) * 128]
                eout[j, h * 8:h * 8 + 8, s * MAIN:(s + 1) * MAIN, :] = lanes[:HALF_MAIN].reshape(8, MAIN, 128)
                rests += jnp.dot(gather(s), lanes[HALF_MAIN:], preferred_element_type=F32)
        eout[j, h * 8:h * 8 + 8, GROUPS * MAIN:, :] = rests.astype(BF).reshape(8, 16, 128)
        for q, dx, dy in partners:
            if q // 8 == h:
                back_to = device((x + 4 - dx) % 4, (y + 8 - dy) % 8, z, core)
                remote(eout.at[j, q], back.at[j, q], ret_send.at[j], ret_recv.at[j], back_to).start()
        if h == SELF // 8:
            back[j, SELF] = eout[j, SELF]

    ring_turn(1, (0, 1))
    ring_turn(2, (0, 1))
    own_turn(2)
    near = [z, (z + 7) % 8, (z + 1) % 8, (z + 6) % 8, (z + 2) % 8, (z + 5) % 8, (z + 3) % 8]
    opposite = (z + 4) % 8
    for origin in near:
        crossed(origin)
    unpack(0)
    gacc[...] = product(0, 0, near)
    uacc[...] = product(0, 1, near)
    ring_turn(3, (0, 1))
    crossed(opposite)
    activate(0, gacc[...] + product(0, 0, [opposite]), uacc[...] + product(0, 1, [opposite]))
    ring_turn(0, (2,))
    columns(0, 0)
    unpack(1)
    gacc[...] = product(1, 0, near + [opposite])
    activate(1, gacc[...], product(1, 1, near + [opposite]))
    columns(0, 1)
    ring_turn(1, (2,))
    columns(1, 0)
    columns(1, 1)
    ring_turn(2, (2,))
    columns(2, 0)
    columns(2, 1)
    ring_turn(3, (2,))
    columns(3, 0)
    columns(3, 1)

    squares = jnp.zeros((TOK, 1), F32)
    for j in range(4):
        pltpu.make_async_copy(back.at[j, 0:15], back.at[j, 0:15], ret_recv.at[j]).wait()
        last = back[j, :, GROUPS * MAIN:, :].reshape(256, 128)
        main = jnp.concatenate(
            [back[j, :, s * MAIN:(s + 1) * MAIN, :].reshape(16 * MAIN, 128) for s in range(4)], axis=1
        )
        total = jnp.dot(whi[...], main, preferred_element_type=F32)
        total += jnp.dot(wlo[...], main, preferred_element_type=F32)
        total += jnp.concatenate(
            [
                jnp.dot(thi[s], last, preferred_element_type=F32) + jnp.dot(tlo[s], last, preferred_element_type=F32)
                for s in range(4)
            ],
            axis=1,
        )
        for half, origin in enumerate(pair(j)):
            at = pl.ds(pl.multiple_of(origin * 256, 256), 256)
            mixed = tok[:, at] + total[:, half * 256:(half + 1) * 256]
            squares += jnp.sum(mixed * mixed, axis=1, keepdims=True)
            tok[:, at] = mixed
            pltpu.make_async_copy(tok.at[:, at], mixed_hbm.at[:, at], res_sem).start()
    scale_ref[...] = lax.rsqrt(squares * (1.0 / WIDTH) + 1e-06)
    pltpu.make_async_copy(tok, mixed_hbm, res_sem).wait()

    @pl.when(home)
    def _():
        pltpu.make_async_copy(wgu.at[0], wgu.at[0], pre_send.at[0]).wait()
        pltpu.make_async_copy(wd.at[0], wd.at[0], pre_send.at[1]).wait()

    @pl.when(jnp.logical_not(home))
    def _():
        pltpu.make_async_copy(wgu.at[0:2], wgu.at[0:2], pre_send.at[0]).wait()
        pltpu.make_async_copy(wd.at[0:2], wd.at[0:2], pre_send.at[1]).wait()

    pltpu.make_async_copy(wgu.at[0:14], wgu.at[0:14], ring_send.at[0]).wait()
    pltpu.make_async_copy(wd.at[0:14], wd.at[0:14], ring_send.at[1]).wait()
    pltpu.make_async_copy(wgu.at[0:16], wgu.at[0:16], sib_send.at[0]).wait()
    pltpu.make_async_copy(wd.at[0:16], wd.at[0:16], sib_send.at[1]).wait()
    pltpu.make_async_copy(send.at[0:15], send.at[0:15], out_send).wait()
    for j in range(4):
        pltpu.make_async_copy(eout.at[j, 0:15], eout.at[j, 0:15], ret_send.at[j]).wait()


def on_device(tokens, expert_ids, combine_weights, gate_weight, up_weight, down_weight, norm_gain):
    hbm = pl.BlockSpec(memory_space=pltpu.HBM)
    vmem = pl.BlockSpec(memory_space=pltpu.VMEM)
    dma = pltpu.SemaphoreType.DMA
    mixed, scale = pl.pallas_call(
        kernel,
        out_shape=(jax.ShapeDtypeStruct((TOK, WIDTH), F32), jax.ShapeDtypeStruct((TOK, 1), F32)),
        in_specs=[hbm] * 6,
        out_specs=(hbm, vmem),
        scratch_shapes=[
            pltpu.VMEM((TOK, WIDTH), F32),
            pltpu.VMEM((2, TOK), jnp.int32),
            pltpu.VMEM((2, TOK), F32),
            pltpu.VMEM((32, 2 * SHARD, FF), BF),
            pltpu.VMEM((32, SHARD, FF), BF),
            pltpu.VMEM((16, ROWS, COLS), BF),
            pltpu.VMEM((16, ROWS, COLS), BF),
            pltpu.VMEM((8, 16 * CAP, 256), BF),
            pltpu.VMEM((HALF, FF), F32),
            pltpu.VMEM((HALF, FF), F32),
            pltpu.VMEM((16 * CAP, FF), BF),
            pltpu.VMEM((4, 16, ROWS, 128), BF),
            pltpu.VMEM((4, 16, ROWS, 128), BF),
            pltpu.VMEM((TOK, 16 * MAIN), BF),
            pltpu.VMEM((TOK, 16 * MAIN), BF),
            pltpu.VMEM((GROUPS, TOK, 256), BF),
            pltpu.VMEM((GROUPS, TOK, 256), BF),
            dma((3,)), dma, dma((2,)), dma((2, PIECES)), dma((2,)), dma((32,)), dma((16,)), dma((2,)), dma((8,)), dma((8,)),
            dma, dma((2,)), dma((4,)), dma((4,)),
        ],
        compiler_params=pltpu.CompilerParams(
            collective_id=0, has_side_effects=True, vmem_limit_bytes=62500000
        ),
        cost_estimate=pl.CostEstimate(flops=7_000_000_000, bytes_accessed=30_000_000, transcendentals=500_000),
    )(tokens, expert_ids.T, combine_weights.T, gate_weight, up_weight, down_weight)
    return mixed * scale * norm_gain[None, :]


def solution(mesh):
    placed = (
        P(("replica", "expert"), None),
        P(("replica", "expert"), None),
        P(("replica", "expert"), None),
        P("expert", "replica", None),
        P("expert", "replica", None),
        P("expert", "replica", None),
        P(),
    )
    return jax.shard_map(
        on_device,
        mesh=mesh,
        in_specs=placed,
        out_specs=P(("replica", "expert"), None),
        check_vma=False,
    )
```

```python
import jax
import jax.numpy as jnp
from jax import lax
from jax.experimental import pallas as pl
from jax.experimental.pallas import tpu as pltpu
from jax.sharding import PartitionSpec as P

MESH = pl.DeviceIdType.MESH
BF = jnp.bfloat16
F32 = jnp.float32

TOK = 192
WIDTH = 2048
FF = 768
CAP = 36
MAIN = 32
TAIL = CAP - MAIN
GROUPS = 4
COLS = WIDTH // GROUPS
ROWS = GROUPS * CAP
SHARD = 64
PIECES = 3
SELF = 12
HALF = 8 * CAP
HALF_MAIN = 8 * MAIN
HALF_TAIL = 8 * TAIL


def hop_y(k, dx):
    far = 2 if dx < 2 else 6
    one = k * (2 - k) * (3 - k) // 2
    two = k * (k - 1) * (3 - k) // 2
    three = k * (k - 1) * (k - 2) // 6
    return one + 7 * two + far * three


def where_am_i():
    r = lax.axis_index("replica")
    e = lax.axis_index("expert")
    z = r // 4
    xh = (r // 2) % 2
    core = r % 2
    xl = e // 8
    y = e % 8
    return xh * 2 + xl, y, z, core


def device(x, y, z, core):
    return ((z * 2 + x // 2) * 2 + core, (x % 2) * 8 + y)


def partner_of(ids, x, y):
    host_x = (ids >> 3) + 2 * ((ids >> 2) & 1)
    dx = (host_x - x) & 3
    d4 = ((ids & 3) - y) & 3
    k = d4 ^ (d4 >> 1)
    return ((k - dx - 1) & 3) * 4 + dx


def iota(shape, dim):
    return lax.broadcasted_iota(jnp.int32, shape, dim)


def kernel(
    tok_hbm, ids_hbm, cw_hbm, gate_hbm, up_hbm, down_hbm, gain_hbm,
    out_ref,
    tok, ids_ref, cw_ref, gain_ref, wgu, wd, send, recv, lhs, gacc, uacc, hid, eout, back, whi, wlo, thi, tlo,
    in_sem, pre_send, pre_recv, ring_send, ring_recv, down_recv, sib_send, sib_gu, sib_down,
    out_send, out_recv, ret_send, ret_recv,
):
    x, y, z, core = where_am_i()
    xh = x // 2
    mine = z * 4 + xh * 2 + core
    home = xh == y // 4
    shards = (gate_hbm, up_hbm, down_hbm)

    ids_copy = pltpu.make_async_copy(ids_hbm, ids_ref, in_sem.at[0])
    cw_copy = pltpu.make_async_copy(cw_hbm, cw_ref, in_sem.at[1])
    tok_copy = pltpu.make_async_copy(tok_hbm, tok, in_sem.at[2])
    ids_copy.start()
    cw_copy.start()
    tok_copy.start()
    gain_copy = pltpu.make_async_copy(gain_hbm, gain_ref, in_sem.at[3])
    gain_copy.start()

    offsets = [(dx, dy) for dx in range(4) for dy in (0, 1, 7)]
    offsets += [(0, 2), (0, 6), (1, 2), (2, 2), (2, 6), (3, 6)]
    offsets += [(0, 4), (2, 4)]
    greet = [device((x + dx) % 4, (y + dy) % 8, z, core) for dx, dy in offsets if (dx, dy) != (0, 0)]
    other = device(x, y, z, 1 - core)
    sides = (device(x, y, (z + 1) % 8, core), device(x, y, (z + 7) % 8, core))
    greet += [other, sides[0], sides[1]]
    barrier = pltpu.get_barrier_semaphore()
    for d in greet:
        pl.semaphore_signal(barrier, inc=1, device_id=d, device_id_type=MESH)
    pl.semaphore_wait(barrier, len(greet))

    def piece(slot, p):
        return wd.at[slot] if p == 2 else wgu.at[slot, pl.ds(p * SHARD, SHARD), :]

    def remote(src, dst, sem_from, sem_to, d):
        return pltpu.make_async_remote_copy(
            src_ref=src, dst_ref=dst, send_sem=sem_from, recv_sem=sem_to, device_id=d, device_id_type=MESH
        )

    def push_own(p, d):
        remote(shards[p].at[0], piece(mine, p), pre_send.at[p // 2], pre_recv.at[xh, p], d).start()

    @pl.when(home)
    def _():
        for p in range(PIECES):
            pltpu.make_async_copy(shards[p].at[0], piece(mine, p), pre_recv.at[xh, p]).start()
            push_own(p, device(x, (y + 4) % 8, z, core))

    @pl.when(jnp.logical_not(home))
    def _():
        for p in range(PIECES):
            push_own(p, device((x + 2) % 4, (y + 4) % 8, z, core))
            push_own(p, device((x + 2) % 4, y, z, core))

    ids_copy.wait()
    cw_copy.wait()
    tok_copy.wait()
    gain_copy.wait()
    q0 = partner_of(ids_ref[0:1, :], x, y)
    q1 = partner_of(ids_ref[1:2, :], x, y)
    hot0 = (q0 == iota((16, TOK), 0)).astype(F32)
    hot1 = (q1 == iota((16, TOK), 0)).astype(F32)
    upper = (iota((TOK, TOK), 0) < iota((TOK, TOK), 1)).astype(BF)
    count = jnp.dot((hot0 + hot1).astype(BF), upper, preferred_element_type=F32)
    rank0 = jnp.sum(hot0 * count, axis=0, keepdims=True).astype(jnp.int32)
    rank1 = jnp.sum(hot1 * count, axis=0, keepdims=True).astype(jnp.int32)
    main0 = jnp.where(rank0 < MAIN, q0 * MAIN + rank0, -1)
    main1 = jnp.where(rank1 < MAIN, q1 * MAIN + rank1, -1)
    tail0 = jnp.where(rank0 < MAIN, -1000, q0 * 16 + rank0 - MAIN)
    tail1 = jnp.where(rank1 < MAIN, -1000, q1 * 16 + rank1 - MAIN)
    select = jnp.where((main0 == iota((16 * MAIN, TOK), 0)) | (main1 == iota((16 * MAIN, TOK), 0)), 1.0, 0.0).astype(BF)
    tails = jnp.zeros((256, COLS), F32)
    for c in range(GROUPS):
        tok_c = tok[:, c * COLS:(c + 1) * COLS].astype(BF)
        placed = jnp.dot(select, tok_c, preferred_element_type=F32).astype(BF)
        send[:, c * MAIN:(c + 1) * MAIN, :] = placed.reshape(16, MAIN, COLS)
        at = iota((256, TOK), 0) - 4 * c
        pick = jnp.where((tail0 == at) | (tail1 == at), 1.0, 0.0).astype(BF)
        tails += jnp.dot(pick, tok_c, preferred_element_type=F32)
    send[:, GROUPS * MAIN:, :] = tails.astype(BF).reshape(16, 16, COLS)

    partners = []
    for g in range(4):
        for dx in range(4):
            dy = hop_y((g + 1 + dx) % 4, dx)
            if (dx, dy) != (0, 0):
                partners.append((g * 4 + dx, dx, dy))
    for q, dx, dy in partners:
        remote(send.at[q], recv.at[q], out_send, out_recv.at[q // 8], device((x + dx) % 4, (y + dy) % 8, z, core)).start()
    recv[SELF] = send[SELF]

    def arrival(step, way, hx, p):
        if p == 2:
            return down_recv.at[(step * 2 + way) * 2 + hx]
        return ring_recv.at[((step * 2 + way) * 2 + hx) * 2 + p]

    def onward(step, way, hx, p, slot):
        return remote(piece(slot, p), piece(slot, p), ring_send.at[p // 2], arrival(step, way, hx, p), sides[way])

    def sibling(p, slot, from_z):
        sem = sib_down.at[from_z] if p == 2 else sib_gu.at[from_z]
        remote(piece(slot, p), piece(slot, p), sib_send.at[p // 2], sem, other).start()

    def own_turn(p):
        for turn in range(2):
            hx = xh if turn == 0 else 1 - xh
            slot = z * 4 + hx * 2 + core
            pltpu.make_async_copy(piece(slot, p), piece(slot, p), pre_recv.at[hx, p]).wait()
            for way in range(2):
                onward(0, way, hx, p, slot).start()
            sibling(p, slot, z)

    def ring_turn(step, pieces):
        for p in pieces:
            for hx in range(2):
                for way in range(2):
                    if step == 3 and way != hx:
                        continue
                    origin = (z + (7 - step if way == 0 else 1 + step)) % 8
                    slot = origin * 4 + hx * 2 + core
                    onward(step, way, hx, p, slot).wait_recv()
                    if step < 2 or (step == 2 and way == hx):
                        onward(step + 1, way, hx, p, slot).start()
                    sibling(p, slot, origin)

    own_turn(0)
    own_turn(1)
    ring_turn(0, (0, 1))

    diagonal = iota((TOK, TOK), 0) == iota((TOK, TOK), 1)

    def column(row):
        return jnp.sum(jnp.where(diagonal, row, 0.0), axis=1, keepdims=True)

    cw0 = column(cw_ref[0:1, :])
    cw1 = column(cw_ref[1:2, :])
    cmain0 = column(main0.astype(F32)).astype(jnp.int32)
    cmain1 = column(main1.astype(F32)).astype(jnp.int32)
    ctail0 = column(tail0.astype(F32)).astype(jnp.int32)
    ctail1 = column(tail1.astype(F32)).astype(jnp.int32)
    slots = iota((TOK, 16 * MAIN), 1)
    full = jnp.where(cmain0 == slots, cw0, 0.0) + jnp.where(cmain1 == slots, cw1, 0.0)
    high = full.astype(BF)
    whi[...] = high
    wlo[...] = (full - high.astype(F32)).astype(BF)
    for c in range(GROUPS):
        slots = iota((TOK, 256), 1) - 4 * c
        full = jnp.where(ctail0 == slots, cw0, 0.0) + jnp.where(ctail1 == slots, cw1, 0.0)
        high = full.astype(BF)
        thi[c] = high
        tlo[c] = (full - high.astype(F32)).astype(BF)

    def spread(c):
        a = iota((HALF_TAIL, 128), 0)
        b = iota((HALF_TAIL, 128), 1)
        return jnp.where((a // 4 == b // 16) & (a % 4 == b % 4) & ((b // 4) % 4 == c), 1.0, 0.0).astype(BF)

    def unpack(h):
        got = recv.at[0:8 - h]
        pltpu.make_async_copy(got, got, out_recv.at[h]).wait()
        last = recv[h * 8:h * 8 + 8, GROUPS * MAIN:, :].reshape(128, COLS)
        for c in range(GROUPS):
            main = recv[h * 8:h * 8 + 8, c * MAIN:(c + 1) * MAIN, :].reshape(HALF_MAIN, COLS)
            rest = jnp.dot(spread(c), last, preferred_element_type=F32).astype(BF)
            for part in range(2):
                lanes = slice(part * 256, (part + 1) * 256)
                lhs[c * 2 + part, h * HALF:h * HALF + HALF_MAIN, :] = main[:, lanes]
                lhs[c * 2 + part, h * HALF + HALF_MAIN:(h + 1) * HALF, :] = rest[:, lanes]

    def weights_of(origin, p):
        at = pl.ds(pl.multiple_of(origin * 4, 4), 4)
        return wgu[at, p * SHARD:(p + 1) * SHARD, :].reshape(256, FF)

    def product(h, p, origins):
        rows = jnp.concatenate([lhs[o, h * HALF:(h + 1) * HALF, :] for o in origins], axis=1)
        return jnp.dot(rows, jnp.concatenate([weights_of(o, p) for o in origins], axis=0), preferred_element_type=F32)

    def activate(h, gate, upward):
        hid[h * HALF:(h + 1) * HALF, :] = (gate / (1.0 + jnp.exp(-gate)) * upward).astype(BF)

    def crossed(origin):
        pltpu.make_async_copy(wgu.at[0:2], wgu.at[0:2], sib_gu.at[origin]).wait()

    def pair(j):
        return ((z + (7 - j)) % 8, (z + 1 + j) % 8) if j < 3 else (z, (z + 4) % 8)

    def gather(s):
        a = iota((128, HALF_TAIL), 0)
        b = iota((128, HALF_TAIL), 1)
        return jnp.where((a // 16 == b // 4) & (a % 4 == b % 4) & ((a // 4) % 4 == s), 1.0, 0.0).astype(BF)

    def columns(j, h):
        rests = jnp.zeros((128, 128), F32)
        for half, origin in enumerate(pair(j)):
            if h == 0:
                pltpu.make_async_copy(wd.at[0:2], wd.at[0:2], sib_down.at[origin]).wait()
            down = wd[pl.ds(pl.multiple_of(origin * 4, 4), 4)].reshape(256, FF)
            res = lax.dot_general(
                hid[h * HALF:(h + 1) * HALF, :], down, (((1,), (1,)), ((), ())), preferred_element_type=F32
            ).astype(BF)
            for part in range(2):
                s = half * 2 + part
                lanes = res[:, part * 128:(part + 1) * 128]
                eout[j, h * 8:h * 8 + 8, s * MAIN:(s + 1) * MAIN, :] = lanes[:HALF_MAIN].reshape(8, MAIN, 128)
                rests += jnp.dot(gather(s), lanes[HALF_MAIN:], preferred_element_type=F32)
        eout[j, h * 8:h * 8 + 8, GROUPS * MAIN:, :] = rests.astype(BF).reshape(8, 16, 128)
        for q, dx, dy in partners:
            if q // 8 == h:
                back_to = device((x + 4 - dx) % 4, (y + 8 - dy) % 8, z, core)
                remote(eout.at[j, q], back.at[j, q], ret_send.at[j], ret_recv.at[j], back_to).start()
        if h == SELF // 8:
            back[j, SELF] = eout[j, SELF]

    ring_turn(1, (0, 1))
    ring_turn(2, (0, 1))
    own_turn(2)
    near = [z, (z + 7) % 8, (z + 1) % 8, (z + 6) % 8, (z + 2) % 8, (z + 5) % 8, (z + 3) % 8]
    opposite = (z + 4) % 8
    for origin in near:
        crossed(origin)
    unpack(0)
    gacc[...] = product(0, 0, near)
    uacc[...] = product(0, 1, near)
    ring_turn(3, (0, 1))
    crossed(opposite)
    activate(0, gacc[...] + product(0, 0, [opposite]), uacc[...] + product(0, 1, [opposite]))
    ring_turn(0, (2,))
    columns(0, 0)
    unpack(1)
    gacc[...] = product(1, 0, near + [opposite])
    activate(1, gacc[...], product(1, 1, near + [opposite]))
    columns(0, 1)
    ring_turn(1, (2,))
    columns(1, 0)
    columns(1, 1)
    ring_turn(2, (2,))
    columns(2, 0)
    columns(2, 1)
    ring_turn(3, (2,))
    columns(3, 0)
    columns(3, 1)

    squares = jnp.zeros((TOK, 1), F32)
    for j in range(4):
        pltpu.make_async_copy(back.at[j, 0:15], back.at[j, 0:15], ret_recv.at[j]).wait()
        last = back[j, :, GROUPS * MAIN:, :].reshape(256, 128)
        main = jnp.concatenate(
            [back[j, :, s * MAIN:(s + 1) * MAIN, :].reshape(16 * MAIN, 128) for s in range(4)], axis=1
        )
        total = jnp.dot(whi[...], main, preferred_element_type=F32)
        total += jnp.dot(wlo[...], main, preferred_element_type=F32)
        total += jnp.concatenate(
            [
                jnp.dot(thi[s], last, preferred_element_type=F32) + jnp.dot(tlo[s], last, preferred_element_type=F32)
                for s in range(4)
            ],
            axis=1,
        )
        for half, origin in enumerate(pair(j)):
            at = pl.ds(pl.multiple_of(origin * 256, 256), 256)
            mixed = tok[:, at] + total[:, half * 256:(half + 1) * 256]
            squares += jnp.sum(mixed * mixed, axis=1, keepdims=True)
            out_ref[:, at] = mixed
    scale = lax.rsqrt(squares * (1.0 / WIDTH) + 1e-06)
    for c in range(GROUPS):
        lanes = slice(c * COLS, (c + 1) * COLS)
        out_ref[:, lanes] = out_ref[:, lanes] * scale * gain_ref[:, lanes]

    @pl.when(home)
    def _():
        pltpu.make_async_copy(wgu.at[0], wgu.at[0], pre_send.at[0]).wait()
        pltpu.make_async_copy(wd.at[0], wd.at[0], pre_send.at[1]).wait()

    @pl.when(jnp.logical_not(home))
    def _():
        pltpu.make_async_copy(wgu.at[0:2], wgu.at[0:2], pre_send.at[0]).wait()
        pltpu.make_async_copy(wd.at[0:2], wd.at[0:2], pre_send.at[1]).wait()

    pltpu.make_async_copy(wgu.at[0:14], wgu.at[0:14], ring_send.at[0]).wait()
    pltpu.make_async_copy(wd.at[0:14], wd.at[0:14], ring_send.at[1]).wait()
    pltpu.make_async_copy(wgu.at[0:16], wgu.at[0:16], sib_send.at[0]).wait()
    pltpu.make_async_copy(wd.at[0:16], wd.at[0:16], sib_send.at[1]).wait()
    pltpu.make_async_copy(send.at[0:15], send.at[0:15], out_send).wait()
    for j in range(4):
        pltpu.make_async_copy(eout.at[j, 0:15], eout.at[j, 0:15], ret_send.at[j]).wait()


def on_device(tokens, expert_ids, combine_weights, gate_weight, up_weight, down_weight, norm_gain):
    hbm = pl.BlockSpec(memory_space=pltpu.HBM)
    vmem = pl.BlockSpec(memory_space=pltpu.VMEM)
    dma = pltpu.SemaphoreType.DMA
    return pl.pallas_call(
        kernel,
        out_shape=jax.ShapeDtypeStruct((TOK, WIDTH), F32),
        in_specs=[hbm] * 7,
        out_specs=vmem,
        scratch_shapes=[
            pltpu.VMEM((TOK, WIDTH), F32),
            pltpu.VMEM((2, TOK), jnp.int32),
            pltpu.VMEM((2, TOK), F32),
            pltpu.VMEM((1, WIDTH), F32),
            pltpu.VMEM((32, 2 * SHARD, FF), BF),
            pltpu.VMEM((32, SHARD, FF), BF),
            pltpu.VMEM((16, ROWS, COLS), BF),
            pltpu.VMEM((16, ROWS, COLS), BF),
            pltpu.VMEM((8, 16 * CAP, 256), BF),
            pltpu.VMEM((HALF, FF), F32),
            pltpu.VMEM((HALF, FF), F32),
            pltpu.VMEM((16 * CAP, FF), BF),
            pltpu.VMEM((4, 16, ROWS, 128), BF),
            pltpu.VMEM((4, 16, ROWS, 128), BF),
            pltpu.VMEM((TOK, 16 * MAIN), BF),
            pltpu.VMEM((TOK, 16 * MAIN), BF),
            pltpu.VMEM((GROUPS, TOK, 256), BF),
            pltpu.VMEM((GROUPS, TOK, 256), BF),
            dma((4,)), dma((2,)), dma((2, PIECES)), dma((2,)), dma((32,)), dma((16,)), dma((2,)), dma((8,)), dma((8,)),
            dma, dma((2,)), dma((4,)), dma((4,)),
        ],
        compiler_params=pltpu.CompilerParams(
            collective_id=0, has_side_effects=True, vmem_limit_bytes=48000000
        ),
        cost_estimate=pl.CostEstimate(flops=7_000_000_000, bytes_accessed=30_000_000, transcendentals=500_000),
    )(*[pltpu.with_memory_space_constraint(v, pltpu.HBM) for v in (tokens, expert_ids.T, combine_weights.T, gate_weight, up_weight, down_weight, norm_gain[None, :])])


def solution(mesh):
    placed = (
        P(("replica", "expert"), None),
        P(("replica", "expert"), None),
        P(("replica", "expert"), None),
        P("expert", "replica", None),
        P("expert", "replica", None),
        P("expert", "replica", None),
        P(),
    )
    return jax.shard_map(
        on_device,
        mesh=mesh,
        in_specs=placed,
        out_specs=P(("replica", "expert"), None),
        check_vma=False,
    )
```

```python
import jax
import jax.numpy as jnp
from jax import lax
from jax.experimental import pallas as pl
from jax.experimental.pallas import tpu as pltpu
from jax.sharding import PartitionSpec as P

MESH = pl.DeviceIdType.MESH
BF = jnp.bfloat16
F32 = jnp.float32

TOK = 192
WIDTH = 2048
FF = 768
CAP = 36
MAIN = 32
TAIL = CAP - MAIN
GROUPS = 4
COLS = WIDTH // GROUPS
ROWS = GROUPS * CAP
SHARD = 64
PIECES = 3
SELF = 12
HALF = 8 * CAP
HALF_MAIN = 8 * MAIN
HALF_TAIL = 8 * TAIL


def hop_y(k, dx):
    far = 2 if dx < 2 else 6
    one = k * (2 - k) * (3 - k) // 2
    two = k * (k - 1) * (3 - k) // 2
    three = k * (k - 1) * (k - 2) // 6
    return one + 7 * two + far * three


def where_am_i():
    r = lax.axis_index("replica")
    e = lax.axis_index("expert")
    z = r // 4
    xh = (r // 2) % 2
    core = r % 2
    xl = e // 8
    y = e % 8
    return xh * 2 + xl, y, z, core


def device(x, y, z, core):
    return ((z * 2 + x // 2) * 2 + core, (x % 2) * 8 + y)


def partner_of(ids, x, y):
    host_x = (ids >> 3) + 2 * ((ids >> 2) & 1)
    dx = (host_x - x) & 3
    d4 = ((ids & 3) - y) & 3
    k = d4 ^ (d4 >> 1)
    return ((k - dx - 1) & 3) * 4 + dx


def iota(shape, dim):
    return lax.broadcasted_iota(jnp.int32, shape, dim)


def kernel(
    tok_hbm, ids_hbm, cw_hbm, gate_hbm, up_hbm, down_hbm, gain_hbm,
    out_ref,
    tok, ids_ref, cw_ref, gain_ref, wgu, wd, send, recv, lhs, gacc, uacc, hid, eout, back, whi, wlo, thi, tlo,
    in_sem, pre_send, pre_recv, ring_send, ring_recv, down_recv, sib_send, sib_gu, sib_down,
    out_send, out_recv, ret_send, ret_recv,
):
    x, y, z, core = where_am_i()
    xh = x // 2
    mine = z * 4 + xh * 2 + core
    home = xh == y // 4
    shards = (gate_hbm, up_hbm, down_hbm)

    ids_copy = pltpu.make_async_copy(ids_hbm, ids_ref, in_sem.at[0])
    cw_copy = pltpu.make_async_copy(cw_hbm, cw_ref, in_sem.at[1])
    tok_copy = pltpu.make_async_copy(tok_hbm, tok, in_sem.at[2])
    ids_copy.start()
    cw_copy.start()
    tok_copy.start()
    gain_copy = pltpu.make_async_copy(gain_hbm, gain_ref, in_sem.at[3])
    gain_copy.start()

    offsets = [(dx, dy) for dx in range(4) for dy in (0, 1, 7)]
    offsets += [(0, 2), (0, 6), (1, 2), (2, 2), (2, 6), (3, 6)]
    offsets += [(0, 4), (2, 4)]
    greet = [device((x + dx) % 4, (y + dy) % 8, z, core) for dx, dy in offsets if (dx, dy) != (0, 0)]
    other = device(x, y, z, 1 - core)
    sides = (device(x, y, (z + 1) % 8, core), device(x, y, (z + 7) % 8, core))
    greet += [other, sides[0], sides[1]]
    barrier = pltpu.get_barrier_semaphore()
    for d in greet:
        pl.semaphore_signal(barrier, inc=1, device_id=d, device_id_type=MESH)
    pl.semaphore_wait(barrier, len(greet))

    def piece(slot, p):
        return wd.at[slot] if p == 2 else wgu.at[slot, pl.ds(p * SHARD, SHARD), :]

    def remote(src, dst, sem_from, sem_to, d):
        return pltpu.make_async_remote_copy(
            src_ref=src, dst_ref=dst, send_sem=sem_from, recv_sem=sem_to, device_id=d, device_id_type=MESH
        )

    def push_own(p, d):
        remote(shards[p].at[0], piece(mine, p), pre_send.at[p // 2], pre_recv.at[xh, p], d).start()

    @pl.when(home)
    def _():
        for p in range(PIECES):
            pltpu.make_async_copy(shards[p].at[0], piece(mine, p), pre_recv.at[xh, p]).start()
            push_own(p, device(x, (y + 4) % 8, z, core))

    @pl.when(jnp.logical_not(home))
    def _():
        for p in range(PIECES):
            push_own(p, device((x + 2) % 4, (y + 4) % 8, z, core))
            push_own(p, device((x + 2) % 4, y, z, core))

    ids_copy.wait()
    cw_copy.wait()
    tok_copy.wait()
    gain_copy.wait()
    q0 = partner_of(ids_ref[0:1, :], x, y)
    q1 = partner_of(ids_ref[1:2, :], x, y)
    hot0 = (q0 == iota((16, TOK), 0)).astype(F32)
    hot1 = (q1 == iota((16, TOK), 0)).astype(F32)
    upper = (iota((TOK, TOK), 0) < iota((TOK, TOK), 1)).astype(BF)
    count = jnp.dot((hot0 + hot1).astype(BF), upper, preferred_element_type=F32)
    rank0 = jnp.sum(hot0 * count, axis=0, keepdims=True).astype(jnp.int32)
    rank1 = jnp.sum(hot1 * count, axis=0, keepdims=True).astype(jnp.int32)
    main0 = jnp.where(rank0 < MAIN, q0 * MAIN + rank0, -1)
    main1 = jnp.where(rank1 < MAIN, q1 * MAIN + rank1, -1)
    tail0 = jnp.where(rank0 < MAIN, -1000, q0 * 16 + rank0 - MAIN)
    tail1 = jnp.where(rank1 < MAIN, -1000, q1 * 16 + rank1 - MAIN)
    select = jnp.where((main0 == iota((16 * MAIN, TOK), 0)) | (main1 == iota((16 * MAIN, TOK), 0)), 1.0, 0.0).astype(BF)
    tails = jnp.zeros((256, COLS), F32)
    for c in range(GROUPS):
        tok_c = tok[:, c * COLS:(c + 1) * COLS].astype(BF)
        placed = jnp.dot(select, tok_c, preferred_element_type=F32).astype(BF)
        send[:, c * MAIN:(c + 1) * MAIN, :] = placed.reshape(16, MAIN, COLS)
        at = iota((256, TOK), 0) - 4 * c
        pick = jnp.where((tail0 == at) | (tail1 == at), 1.0, 0.0).astype(BF)
        tails += jnp.dot(pick, tok_c, preferred_element_type=F32)
    send[:, GROUPS * MAIN:, :] = tails.astype(BF).reshape(16, 16, COLS)

    partners = []
    for g in range(4):
        for dx in range(4):
            dy = hop_y((g + 1 + dx) % 4, dx)
            if (dx, dy) != (0, 0):
                partners.append((g * 4 + dx, dx, dy))
    partners.sort(key=lambda m: (min(m[1], 4 - m[1]), -min(m[2], 8 - m[2])))
    partners = [partners[i // 2] if i % 2 == 0 else partners[-1 - i // 2] for i in range(len(partners))]
    for q, dx, dy in partners:
        remote(send.at[q], recv.at[q], out_send, out_recv.at[q // 8], device((x + dx) % 4, (y + dy) % 8, z, core)).start()
    recv[SELF] = send[SELF]

    def arrival(step, way, hx, p):
        if p == 2:
            return down_recv.at[(step * 2 + way) * 2 + hx]
        return ring_recv.at[((step * 2 + way) * 2 + hx) * 2 + p]

    def onward(step, way, hx, p, slot):
        return remote(piece(slot, p), piece(slot, p), ring_send.at[p // 2], arrival(step, way, hx, p), sides[way])

    def sibling(p, slot, from_z):
        sem = sib_down.at[from_z] if p == 2 else sib_gu.at[from_z]
        remote(piece(slot, p), piece(slot, p), sib_send.at[p // 2], sem, other).start()

    def own_turn(p):
        for turn in range(2):
            hx = xh if turn == 0 else 1 - xh
            slot = z * 4 + hx * 2 + core
            pltpu.make_async_copy(piece(slot, p), piece(slot, p), pre_recv.at[hx, p]).wait()
            for way in range(2):
                onward(0, way, hx, p, slot).start()
            sibling(p, slot, z)

    def ring_turn(step, pieces):
        for p in pieces:
            for hx in range(2):
                for way in range(2):
                    if step == 3 and way != hx:
                        continue
                    origin = (z + (7 - step if way == 0 else 1 + step)) % 8
                    slot = origin * 4 + hx * 2 + core
                    onward(step, way, hx, p, slot).wait_recv()
                    if step < 2 or (step == 2 and way == hx):
                        onward(step + 1, way, hx, p, slot).start()
                    sibling(p, slot, origin)

    own_turn(0)
    own_turn(1)
    ring_turn(0, (0, 1))

    diagonal = iota((TOK, TOK), 0) == iota((TOK, TOK), 1)

    def column(row):
        return jnp.sum(jnp.where(diagonal, row, 0.0), axis=1, keepdims=True)

    cw0 = column(cw_ref[0:1, :])
    cw1 = column(cw_ref[1:2, :])
    cmain0 = column(main0.astype(F32)).astype(jnp.int32)
    cmain1 = column(main1.astype(F32)).astype(jnp.int32)
    ctail0 = column(tail0.astype(F32)).astype(jnp.int32)
    ctail1 = column(tail1.astype(F32)).astype(jnp.int32)
    slots = iota((TOK, 16 * MAIN), 1)
    full = jnp.where(cmain0 == slots, cw0, 0.0) + jnp.where(cmain1 == slots, cw1, 0.0)
    high = full.astype(BF)
    whi[...] = high
    wlo[...] = (full - high.astype(F32)).astype(BF)
    for c in range(GROUPS):
        slots = iota((TOK, 256), 1) - 4 * c
        full = jnp.where(ctail0 == slots, cw0, 0.0) + jnp.where(ctail1 == slots, cw1, 0.0)
        high = full.astype(BF)
        thi[c] = high
        tlo[c] = (full - high.astype(F32)).astype(BF)

    def spread(c):
        a = iota((HALF_TAIL, 128), 0)
        b = iota((HALF_TAIL, 128), 1)
        return jnp.where((a // 4 == b // 16) & (a % 4 == b % 4) & ((b // 4) % 4 == c), 1.0, 0.0).astype(BF)

    def unpack(h):
        got = recv.at[0:8 - h]
        pltpu.make_async_copy(got, got, out_recv.at[h]).wait()
        last = recv[h * 8:h * 8 + 8, GROUPS * MAIN:, :].reshape(128, COLS)
        for c in range(GROUPS):
            main = recv[h * 8:h * 8 + 8, c * MAIN:(c + 1) * MAIN, :].reshape(HALF_MAIN, COLS)
            rest = jnp.dot(spread(c), last, preferred_element_type=F32).astype(BF)
            for part in range(2):
                lanes = slice(part * 256, (part + 1) * 256)
                lhs[c * 2 + part, h * HALF:h * HALF + HALF_MAIN, :] = main[:, lanes]
                lhs[c * 2 + part, h * HALF + HALF_MAIN:(h + 1) * HALF, :] = rest[:, lanes]

    def weights_of(origin, p):
        at = pl.ds(pl.multiple_of(origin * 4, 4), 4)
        return wgu[at, p * SHARD:(p + 1) * SHARD, :].reshape(256, FF)

    def product(h, p, origins):
        rows = jnp.concatenate([lhs[o, h * HALF:(h + 1) * HALF, :] for o in origins], axis=1)
        return jnp.dot(rows, jnp.concatenate([weights_of(o, p) for o in origins], axis=0), preferred_element_type=F32)

    def activate(h, gate, upward):
        hid[h * HALF:(h + 1) * HALF, :] = (gate / (1.0 + jnp.exp(-gate)) * upward).astype(BF)

    def crossed(origin):
        pltpu.make_async_copy(wgu.at[0:2], wgu.at[0:2], sib_gu.at[origin]).wait()

    def pair(j):
        return ((z + (7 - j)) % 8, (z + 1 + j) % 8) if j < 3 else (z, (z + 4) % 8)

    def gather(s):
        a = iota((128, HALF_TAIL), 0)
        b = iota((128, HALF_TAIL), 1)
        return jnp.where((a // 16 == b // 4) & (a % 4 == b % 4) & ((a // 4) % 4 == s), 1.0, 0.0).astype(BF)

    def columns(j, h):
        rests = jnp.zeros((128, 128), F32)
        for half, origin in enumerate(pair(j)):
            if h == 0:
                pltpu.make_async_copy(wd.at[0:2], wd.at[0:2], sib_down.at[origin]).wait()
            down = wd[pl.ds(pl.multiple_of(origin * 4, 4), 4)].reshape(256, FF)
            res = lax.dot_general(
                hid[h * HALF:(h + 1) * HALF, :], down, (((1,), (1,)), ((), ())), preferred_element_type=F32
            ).astype(BF)
            for part in range(2):
                s = half * 2 + part
                lanes = res[:, part * 128:(part + 1) * 128]
                eout[j, h * 8:h * 8 + 8, s * MAIN:(s + 1) * MAIN, :] = lanes[:HALF_MAIN].reshape(8, MAIN, 128)
                rests += jnp.dot(gather(s), lanes[HALF_MAIN:], preferred_element_type=F32)
        eout[j, h * 8:h * 8 + 8, GROUPS * MAIN:, :] = rests.astype(BF).reshape(8, 16, 128)
        for q, dx, dy in partners:
            if q // 8 == h:
                back_to = device((x + 4 - dx) % 4, (y + 8 - dy) % 8, z, core)
                remote(eout.at[j, q], back.at[j, q], ret_send.at[j], ret_recv.at[j], back_to).start()
        if h == SELF // 8:
            back[j, SELF] = eout[j, SELF]

    ring_turn(1, (0, 1))
    ring_turn(2, (0, 1))
    own_turn(2)
    near = [z, (z + 7) % 8, (z + 1) % 8, (z + 6) % 8, (z + 2) % 8, (z + 5) % 8, (z + 3) % 8]
    opposite = (z + 4) % 8
    for origin in near:
        crossed(origin)
    unpack(0)
    gacc[...] = product(0, 0, near)
    uacc[...] = product(0, 1, near)
    ring_turn(3, (0, 1))
    crossed(opposite)
    activate(0, gacc[...] + product(0, 0, [opposite]), uacc[...] + product(0, 1, [opposite]))
    ring_turn(0, (2,))
    columns(0, 0)
    unpack(1)
    gacc[...] = product(1, 0, near + [opposite])
    activate(1, gacc[...], product(1, 1, near + [opposite]))
    columns(0, 1)
    ring_turn(1, (2,))
    columns(1, 0)
    columns(1, 1)
    ring_turn(2, (2,))
    columns(2, 0)
    columns(2, 1)
    ring_turn(3, (2,))
    columns(3, 0)
    columns(3, 1)

    squares = jnp.zeros((TOK, 1), F32)
    for j in range(4):
        pltpu.make_async_copy(back.at[j, 0:15], back.at[j, 0:15], ret_recv.at[j]).wait()
        last = back[j, :, GROUPS * MAIN:, :].reshape(256, 128)
        main = jnp.concatenate(
            [back[j, :, s * MAIN:(s + 1) * MAIN, :].reshape(16 * MAIN, 128) for s in range(4)], axis=1
        )
        total = jnp.dot(whi[...], main, preferred_element_type=F32)
        total += jnp.dot(wlo[...], main, preferred_element_type=F32)
        total += jnp.concatenate(
            [
                jnp.dot(thi[s], last, preferred_element_type=F32) + jnp.dot(tlo[s], last, preferred_element_type=F32)
                for s in range(4)
            ],
            axis=1,
        )
        for half, origin in enumerate(pair(j)):
            at = pl.ds(pl.multiple_of(origin * 256, 256), 256)
            mixed = tok[:, at] + total[:, half * 256:(half + 1) * 256]
            squares += jnp.sum(mixed * mixed, axis=1, keepdims=True)
            out_ref[:, at] = mixed
    scale = lax.rsqrt(squares * (1.0 / WIDTH) + 1e-06)
    for c in range(GROUPS):
        lanes = slice(c * COLS, (c + 1) * COLS)
        out_ref[:, lanes] = out_ref[:, lanes] * scale * gain_ref[:, lanes]

    @pl.when(home)
    def _():
        pltpu.make_async_copy(wgu.at[0], wgu.at[0], pre_send.at[0]).wait()
        pltpu.make_async_copy(wd.at[0], wd.at[0], pre_send.at[1]).wait()

    @pl.when(jnp.logical_not(home))
    def _():
        pltpu.make_async_copy(wgu.at[0:2], wgu.at[0:2], pre_send.at[0]).wait()
        pltpu.make_async_copy(wd.at[0:2], wd.at[0:2], pre_send.at[1]).wait()

    pltpu.make_async_copy(wgu.at[0:14], wgu.at[0:14], ring_send.at[0]).wait()
    pltpu.make_async_copy(wd.at[0:14], wd.at[0:14], ring_send.at[1]).wait()
    pltpu.make_async_copy(wgu.at[0:16], wgu.at[0:16], sib_send.at[0]).wait()
    pltpu.make_async_copy(wd.at[0:16], wd.at[0:16], sib_send.at[1]).wait()
    pltpu.make_async_copy(send.at[0:15], send.at[0:15], out_send).wait()
    for j in range(4):
        pltpu.make_async_copy(eout.at[j, 0:15], eout.at[j, 0:15], ret_send.at[j]).wait()


def on_device(tokens, expert_ids, combine_weights, gate_weight, up_weight, down_weight, norm_gain):
    hbm = pl.BlockSpec(memory_space=pltpu.HBM)
    vmem = pl.BlockSpec(memory_space=pltpu.VMEM)
    dma = pltpu.SemaphoreType.DMA
    return pl.pallas_call(
        kernel,
        out_shape=jax.ShapeDtypeStruct((TOK, WIDTH), F32),
        in_specs=[hbm] * 7,
        out_specs=vmem,
        scratch_shapes=[
            pltpu.VMEM((TOK, WIDTH), F32),
            pltpu.VMEM((2, TOK), jnp.int32),
            pltpu.VMEM((2, TOK), F32),
            pltpu.VMEM((1, WIDTH), F32),
            pltpu.VMEM((32, 2 * SHARD, FF), BF),
            pltpu.VMEM((32, SHARD, FF), BF),
            pltpu.VMEM((16, ROWS, COLS), BF),
            pltpu.VMEM((16, ROWS, COLS), BF),
            pltpu.VMEM((8, 16 * CAP, 256), BF),
            pltpu.VMEM((HALF, FF), F32),
            pltpu.VMEM((HALF, FF), F32),
            pltpu.VMEM((16 * CAP, FF), BF),
            pltpu.VMEM((4, 16, ROWS, 128), BF),
            pltpu.VMEM((4, 16, ROWS, 128), BF),
            pltpu.VMEM((TOK, 16 * MAIN), BF),
            pltpu.VMEM((TOK, 16 * MAIN), BF),
            pltpu.VMEM((GROUPS, TOK, 256), BF),
            pltpu.VMEM((GROUPS, TOK, 256), BF),
            dma((4,)), dma((2,)), dma((2, PIECES)), dma((2,)), dma((32,)), dma((16,)), dma((2,)), dma((8,)), dma((8,)),
            dma, dma((2,)), dma((4,)), dma((4,)),
        ],
        compiler_params=pltpu.CompilerParams(
            collective_id=0, has_side_effects=True, vmem_limit_bytes=48000000
        ),
        cost_estimate=pl.CostEstimate(flops=7_000_000_000, bytes_accessed=30_000_000, transcendentals=500_000),
    )(*[pltpu.with_memory_space_constraint(v, pltpu.HBM) for v in (tokens, expert_ids.T, combine_weights.T, gate_weight, up_weight, down_weight, norm_gain[None, :])])


def solution(mesh):
    placed = (
        P(("replica", "expert"), None),
        P(("replica", "expert"), None),
        P(("replica", "expert"), None),
        P("expert", "replica", None),
        P("expert", "replica", None),
        P("expert", "replica", None),
        P(),
    )
    return jax.shard_map(
        on_device,
        mesh=mesh,
        in_specs=placed,
        out_specs=P(("replica", "expert"), None),
        check_vma=False,
    )
```
